32 devices in a mesh: leaf: 32 (over z, y, x, core).
Axes of the slice: x: 2, y: 2, z: 4, core: 2. Of those that a mesh axis runs over, the one named last changes fastest.
Arguments:
- features: bfloat16 [16384, 1024], P('leaf'), may hold values from -6 to 6
- probes: float32 [16384, 128], P('leaf'), may hold values from -6 to 6
- bases: float32 [16384, 256], P('leaf'), may hold values from -0.25 to 0.25
- transfers: float32 [32, 4, 256, 256], P('leaf'), may hold values from -1 to 1, as said below
- couplings: float32 [32, 5, 256, 256], P('leaf'), may hold values from -1 to 1, as said below
- near_list: int32 [32, 4], P('leaf'), may hold values from 0 to 31, as said below
- near_count: int32 [32], P('leaf'), may hold values from 1 to 4
Outputs:
- product: float32 [16384, 128], P('leaf')
The draws below stay inside these ranges and needn't reach their ends.
Inputs may be any that keep to these rules, and one draw needn't show every extreme that they name: `near_list`: the first near_count[i] entries of row i are distinct leaves other than i, each at most 2 from i; the other entries equal i. Some leaf lists 4 leaves. transfers[i, l] is the same for all leaves i of one node of level l (an aligned block of 2^l leaves). couplings[i, l] is the same for all leaves i of one node of level l (an aligned block of 2^l leaves).
All inputs are finite; a program needn't handle non-finite values.
Results may differ from the reference program's by a relative error of at most 0.00095.
Values may be sent and summed in bfloat16 or wider, within the bound.
No kernel may reach another device: no remote copies, remote signals or barrier semaphores. Data moves between devices by JAX's collectives and lax.ppermute only.
A program may use at most 64 MiB of HBM per device.

```python
import jax
import jax.numpy as jnp
from jax import lax

ROWS = 512
F = 1024
R = 256
P_SIZE = 128
LEV = 4
SPAN = 2
NEAR_MAX = 4
LEAVES = 32
POINTS = 16384


def near_tables(key):
    span_offsets = jnp.concatenate([jnp.arange(-SPAN, 0), jnp.arange(1, SPAN + 1)]).astype(jnp.int32)
    leaf_ids = jnp.arange(LEAVES, dtype=jnp.int32)
    targets = leaf_ids[:, None] + span_offsets[None, :]
    is_valid = (targets >= 0) & (targets < LEAVES)
    score_key = jax.random.fold_in(key, 11)
    count_key = jax.random.fold_in(key, 12)
    slot_ids = jnp.arange(NEAR_MAX, dtype=jnp.int32)
    scores = jax.random.randint(score_key, (LEAVES, NEAR_MAX), 0, 1 << 16) * NEAR_MAX + slot_ids[None, :]
    scores = jnp.where(is_valid, scores, (1 << 28) + slot_ids[None, :])
    ordering = jnp.argsort(scores, axis=1, stable=True)
    listed = jnp.take_along_axis(targets, ordering, axis=1)
    valid_count = jnp.sum(is_valid.astype(jnp.int32), axis=1)
    wanted = jax.random.randint(count_key, (LEAVES,), 1, NEAR_MAX + 1)
    counts = jnp.minimum(wanted, valid_count)
    counts = jnp.where(leaf_ids == LEAVES // 2, NEAR_MAX, counts)
    listed = jnp.where(slot_ids[None, :] < counts[:, None], listed, leaf_ids[:, None])
    return (listed.astype(jnp.int32), counts.astype(jnp.int32))


def draw_near_list(key, part):
    return near_tables(key)[0]


def draw_near_count(key, part):
    return near_tables(key)[1]


def node_matrices(key, level_count):
    stacked = []
    for height in range(level_count):
        level_key = jax.random.fold_in(key, 100 + height)
        drawn = jax.random.uniform(level_key, (LEAVES // 2 ** height, R, R), jnp.float32, -1.0, 1.0)
        stacked.append(jnp.repeat(drawn, 2 ** height, axis=0))
    return jnp.stack(stacked, axis=1)


def draw_transfers(key, part):
    return node_matrices(jax.random.fold_in(key, 21), LEV)


def draw_couplings(key, part):
    return node_matrices(jax.random.fold_in(key, 22), LEV + 1)


def shard_levels(rng, dims, split, low, high):
    level, own = 1.0, jax.random.fold_in(rng, 6)
    for axis_at, shards_of in split:
        draws = jnp.exp(jax.random.uniform(jax.random.fold_in(own, axis_at), (shards_of,), jnp.float32, low / len(split), high / len(split)))
        level = level * jnp.repeat(draws, dims[axis_at] // shards_of).reshape([-1 if axis == axis_at else 1 for axis in range(len(dims))])
    return level


def noise(stream_key, shape, deviation, reach, cuts=(), kind=jnp.bfloat16):
    values = deviation * jax.random.normal(stream_key, shape, jnp.float32)
    if cuts:
        values = values * shard_levels(stream_key, shape, cuts, -0.22, 0.18)
    return jnp.clip(values, -reach, reach).astype(kind)


def setup_inputs(seed: int = 0) -> dict:
    key_of = jax.random.split(jax.random.key(seed), 8)
    return {
        "features": noise(key_of[0], (POINTS, F), 1.0, 6.0, ((0, 32),)),
        "probes": noise(key_of[1], (POINTS, P_SIZE), 1.0, 6.0, ((0, 32),), jnp.float32),
        "bases": noise(key_of[2], (POINTS, R), ROWS ** -0.5, 0.25, ((0, 32),), jnp.float32),
        "transfers": draw_transfers(jax.random.fold_in(key_of[7], 71), 0),
        "couplings": draw_couplings(jax.random.fold_in(key_of[7], 71), 0),
        "near_list": draw_near_list(jax.random.fold_in(key_of[7], 71), 0),
        "near_count": draw_near_count(jax.random.fold_in(key_of[7], 71), 0),
    }


def kernel_tile(rows_a, rows_b):
    gram_tile = jnp.dot(rows_a, rows_b.T, preferred_element_type=jnp.float32)
    return gram_tile * gram_tile * (1.0 / (F * ROWS))


def sibling(values, height):
    half_block = 2 ** height
    grouped = values.reshape(LEAVES // (2 * half_block), 2, half_block, R, P_SIZE)
    return grouped[:, ::-1].reshape(LEAVES, R, P_SIZE)


def reference(features, probes, bases, transfers, couplings, near_list, near_count):
    highest = lax.Precision.HIGHEST
    scale_g = (3.0 / R) ** 0.5
    leaf_features = features.reshape(LEAVES, ROWS, F)
    leaf_probes = probes.reshape(LEAVES, ROWS, P_SIZE)
    padded_features = jnp.concatenate([leaf_features, jnp.zeros((SPAN, ROWS, F), features.dtype)], 0)
    padded_probes = jnp.concatenate([leaf_probes, jnp.zeros((SPAN, ROWS, P_SIZE), jnp.float32)], 0)
    leaf_ids = jnp.arange(LEAVES, dtype=jnp.int32)
    slot_ids = jnp.arange(NEAR_MAX, dtype=jnp.int32)
    is_live = slot_ids[None, :] < near_count[:, None]

    def member(offset):
        found = (near_list == (leaf_ids + offset)[:, None]) & is_live
        return jnp.any(found, axis=1).astype(jnp.float32)

    def per_leaf(leaf_id):
        own_rows = leaf_features[leaf_id]
        own_probes = leaf_probes[leaf_id]
        outputs = [jnp.dot(kernel_tile(own_rows, own_rows), own_probes, precision=highest, preferred_element_type=jnp.float32)]
        for offset in range(1, SPAN + 1):
            remote = lax.dynamic_index_in_dim(padded_features, leaf_id + offset, 0, keepdims=False)
            remote_x = lax.dynamic_index_in_dim(padded_probes, leaf_id + offset, 0, keepdims=False)
            kernel = kernel_tile(own_rows, remote)
            outputs.append(jnp.dot(kernel, remote_x, precision=highest, preferred_element_type=jnp.float32))
            outputs.append(jnp.dot(kernel.T, own_probes, precision=highest, preferred_element_type=jnp.float32))
        return jnp.stack(outputs)

    pieces = lax.map(per_leaf, leaf_ids)
    near_sum = pieces[:, 0]
    for offset in range(1, SPAN + 1):
        near_sum = near_sum + member(offset)[:, None, None] * pieces[:, 2 * offset - 1]
        back_term = pieces[:, 2 * offset]
        shifted = jnp.concatenate([jnp.zeros((offset, ROWS, P_SIZE), jnp.float32), back_term[:LEAVES - offset]], 0)
        near_sum = near_sum + member(-offset)[:, None, None] * shifted

    leaf_bases = bases.reshape(LEAVES, ROWS, R)
    skeleton = jnp.einsum('nra,nrp->nap', leaf_bases, leaf_probes, precision=highest)
    levels = [skeleton]
    for height in range(1, LEV + 1):
        factor = scale_g * 2.0 ** (-0.5 * height)
        contrib = factor * jnp.einsum('nab,nap->nbp', transfers[:, height - 1], levels[-1], precision=highest)
        levels.append(contrib + sibling(contrib, height - 1))

    expansion = scale_g * jnp.einsum('nab,nbp->nap', couplings[:, LEV], sibling(levels[LEV], LEV), precision=highest)
    for height in range(LEV - 1, -1, -1):
        factor = scale_g * 2.0 ** (-0.5 * (height + 1))
        expansion = scale_g * jnp.einsum('nab,nbp->nap', couplings[:, height], sibling(levels[height], height), precision=highest) + factor * jnp.einsum('nab,nbp->nap', transfers[:, height], expansion, precision=highest)
    far_sum = jnp.einsum('nra,nap->nrp', leaf_bases, expansion, precision=highest)
    return (near_sum + far_sum).reshape(LEAVES * ROWS, P_SIZE)
```

```python
import functools

import jax
import jax.numpy as jnp
from jax import lax
from jax.experimental import pallas as pl
from jax.experimental.pallas import tpu as pltpu
from jax.sharding import PartitionSpec as P

BF16 = jnp.bfloat16
F32 = jnp.float32
VMEM = pl.BlockSpec(memory_space=pltpu.VMEM)
SMEM = pl.BlockSpec(memory_space=pltpu.SMEM)
NN = (((1,), (0,)), ((), ()))
NT = (((1,), (1,)), ((), ()))
TN = (((0,), (0,)), ((), ()))
FLAG_ROWS = 16
LIMIT = 16 << 20


def dot(a, b, dims):
    return lax.dot_general(a, b, dims, preferred_element_type=F32)


def halves(a):
    high = a.astype(BF16)
    return high, (a - high.astype(F32)).astype(BF16)


def dot_wide(a, b, dims):
    a_high, a_low = halves(a)
    b_high, b_low = halves(b)
    return dot(a_high, b_high, dims) + (dot(a_high, b_low, dims) + dot(a_low, b_high, dims))


def dot_half(a16, b, dims):
    b_high, b_low = halves(b)
    return dot(a16, b_high, dims) + dot(a16, b_low, dims)


def member(list_ref, count_ref, offset):
    index = lax.axis_index("leaf")
    found = jnp.float32(0.0)
    for slot in range(list_ref.shape[1]):
        hit = (list_ref[0, slot] == index + offset) & (slot < count_ref[0])
        found = jnp.where(hit, jnp.float32(1.0), found)
    return found


def call(kernel, name, outs, specs, flops, *args):
    out_bytes = sum(o.size * o.dtype.itemsize for o in outs)
    in_bytes = sum(a.size * a.dtype.itemsize for a in args)
    return pl.pallas_call(
        kernel,
        name=name,
        out_shape=outs,
        in_specs=specs,
        out_specs=[VMEM] * len(outs),
        compiler_params=pltpu.CompilerParams(vmem_limit_bytes=LIMIT),
        cost_estimate=pl.CostEstimate(flops=flops, bytes_accessed=in_bytes + out_bytes, transcendentals=0),
    )(*args)


def leaf_kernel(c1, bases_ref, x_ref, transfer_ref, list_ref, count_ref, message_ref, xmessage_ref):
    x = x_ref[...]
    rows, probes = x.shape
    skeleton = dot_wide(x, bases_ref[...], TN)
    message_ref[:probes] = skeleton
    message_ref[probes:] = c1 * dot_wide(skeleton, transfer_ref[0, 0], NN)
    xmessage_ref[:rows] = x.astype(BF16)
    for place, offset in ((0, -2), (1, -1)):
        flag = member(list_ref, count_ref, offset)
        xmessage_ref[rows + place * FLAG_ROWS : rows + (place + 1) * FLAG_ROWS] = jnp.full(
            (FLAG_ROWS, probes), flag, F32
        ).astype(BF16)


def up_kernel(level, factor, own_ref, got_ref, transfer_ref, message_ref, next_ref):
    probes = own_ref.shape[0]
    skeleton = own_ref[...] + got_ref[probes:].astype(F32)
    message_ref[:probes] = skeleton.astype(message_ref.dtype)
    if factor is not None:
        moved = factor * dot_wide(skeleton, transfer_ref[0, level], NN)
        message_ref[probes:] = moved.astype(message_ref.dtype)
        next_ref[...] = moved


def down_kernel(scale_g, factors, got0_ref, *refs):
    depth = len(factors)
    gots = [got0_ref, *refs[:depth]]
    coupling_ref, transfer_ref, bases_ref, out_ref = refs[depth:]
    probes = out_ref.shape[1]
    expansion = None
    for level in range(depth, -1, -1):
        got = gots[level][:probes]
        wide = dot_wide if got.dtype == F32 else dot_half
        update = scale_g * wide(got, coupling_ref[0, level], NT)
        if level < depth:
            update = update + factors[level] * dot_wide(expansion, transfer_ref[0, level], NT)
        expansion = update
    out_ref[...] = dot_wide(bases_ref[...], expansion, NT)


def tile(rows_a, rows_b, scale):
    gram = dot(rows_a, rows_b, NT)
    return halves(gram * gram * scale)


def self_kernel(scale, f_ref, x_ref, out_ref):
    high, low = tile(f_ref[...], f_ref[...], scale)
    x_high, x_low = halves(x_ref[...])
    out_ref[...] = dot(high, x_high, NN) + (dot(high, x_low, NN) + dot(low, x_high, NN))


def times(parts, x16):
    return dot(parts[0], x16, NN) + dot(parts[1], x16, NN)


def times_back(parts, x16):
    return (dot(x16, parts[0], TN) + dot(x16, parts[1], TN)).T


def pair_kernel(scale, f_ref, g_ref, near_ref, x_ref, xs_ref, list_ref, count_ref, out_ref, sib_ref):
    odd = lax.rem(lax.axis_index("leaf"), 2) == 1
    rows = near_ref.shape[0]

    @pl.when(odd)
    def _():
        parts = tile(g_ref[...], f_ref[...], scale)
        sib_ref[...] = times(parts, x_ref[:rows])
        flag = member(list_ref, count_ref, -1)
        out_ref[...] = near_ref[...] + flag * times_back(parts, xs_ref[:rows])

    @pl.when(jnp.logical_not(odd))
    def _():
        out_ref[...] = near_ref[...]
        sib_ref[...] = jnp.zeros_like(sib_ref)


def chunk_kernel(scale, first, f_ref, g_ref, h_ref, near_ref, sib_in_ref, x_ref, xs_ref, xh_ref, list_ref, count_ref, out_ref, sib_ref, back_ref):
    even = lax.rem(lax.axis_index("leaf"), 2) == 0
    rows = near_ref.shape[0]
    size = h_ref.shape[0]
    xh = xh_ref[first : first + size]
    parts = tile(f_ref[...], h_ref[...], scale)
    out_ref[...] = near_ref[...] + member(list_ref, count_ref, 2) * times(parts, xh)
    flag2 = xh_ref[rows : rows + 1].astype(F32)
    flag1 = xh_ref[rows + FLAG_ROWS : rows + FLAG_ROWS + 1].astype(F32)
    back = flag2 * times_back(parts, x_ref[:rows])

    @pl.when(even)
    def _():
        cross = tile(g_ref[...], h_ref[...], scale)
        sib_ref[...] = sib_in_ref[...] + times(cross, xh)
        back_ref[...] = (back + flag1 * times_back(cross, xs_ref[:rows])).astype(BF16)

    @pl.when(jnp.logical_not(even))
    def _():
        sib_ref[...] = sib_in_ref[...]
        back_ref[...] = back.astype(BF16)


def final_kernel(near_ref, far_ref, sib_ref, list_ref, count_ref, *refs):
    out_ref = refs[-1]
    flag = member(list_ref, count_ref, 1)
    at = 0
    for back_ref in refs[:-1]:
        rows = slice(at, at + back_ref.shape[0])
        out_ref[rows] = near_ref[rows] + far_ref[rows] + flag * sib_ref[rows].astype(F32) + back_ref[...].astype(F32)
        at += back_ref.shape[0]


def moved(array, by):
    peers = lax.axis_size("leaf")
    return lax.ppermute(array, "leaf", [(i, i + by) for i in range(peers) if 0 <= i + by < peers])


def partner(array, level):
    return lax.ppermute(array, "leaf", [(i, i ^ 1 << level) for i in range(lax.axis_size("leaf"))])


def chunks_of(rows):
    quarter = rows // 4
    return [(0, quarter), (quarter, quarter), (2 * quarter, quarter), (3 * quarter, quarter)]


def shards(features, probes, bases, transfers, couplings, near_list, near_count):
    rows, width = features.shape
    count = probes.shape[1]
    rank = bases.shape[1]
    depth = transfers.shape[1]
    scale = 1.0 / (rows * width)
    scale_g = (3.0 / rank) ** 0.5
    factors = [scale_g * 2.0 ** (-0.5 * (level + 1)) for level in range(depth)]
    shape = jax.ShapeDtypeStruct

    message, own_x = call(
        functools.partial(leaf_kernel, factors[0]),
        "leaf",
        [shape((2 * count, rank), F32), shape((rows + 2 * FLAG_ROWS, count), BF16)],
        [VMEM] * 3 + [SMEM] * 2,
        6 * rows * rank * count,
        bases, probes, transfers, near_list, near_count,
    )
    sib_features = partner(features, 0)
    sib_x = partner(own_x, 0)
    far_x = moved(own_x, -2)
    pieces = chunks_of(rows)
    far_features = [moved(features[a : a + n], -2) for a, n in pieces]

    gots = [partner(message, 0)]
    own = message[count:]
    for level in range(1, depth + 1):
        last = level == depth
        outs = [shape((count if last else 2 * count, rank), BF16), shape((count, rank), F32)]
        message, own = call(
            functools.partial(up_kernel, level, None if last else factors[level]),
            f"up{level}",
            outs,
            [VMEM] * 3,
            6 * rank * rank * count,
            own, gots[-1], transfers,
        )
        gots.append(partner(message, level))
    (far,) = call(
        functools.partial(down_kernel, scale_g, factors),
        "down",
        [shape((rows, count), F32)],
        [VMEM] * (depth + 4),
        6 * count * rank * (rank * (2 * depth + 1) + rows),
        *gots, couplings, transfers, bases,
    )

    tile_flops = 2 * rows * rows * (width + 4 * count)
    (near,) = call(
        functools.partial(self_kernel, scale),
        "self",
        [shape((rows, count), F32)],
        [VMEM, VMEM],
        tile_flops,
        features, probes,
    )
    near, sib = call(
        functools.partial(pair_kernel, scale),
        "pair",
        [shape((rows, count), F32)] * 2,
        [VMEM] * 5 + [SMEM] * 2,
        tile_flops,
        features, sib_features, near, own_x, sib_x, near_list, near_count,
    )
    backs = []
    for (first, size), part in zip(pieces, far_features):
        near, sib, back = call(
            functools.partial(chunk_kernel, scale, first),
            f"chunk{first}",
            [shape((rows, count), F32), shape((rows, count), F32), shape((size, count), BF16)],
            [VMEM] * 8 + [SMEM] * 2,
            tile_flops * 2 * size // rows,
            features, sib_features, part, near, sib, own_x, sib_x, far_x, near_list, near_count,
        )
        backs.append(moved(back, 2))
    sib_got = partner(sib.astype(BF16), 0)
    (out,) = call(
        final_kernel,
        "final",
        [shape((rows, count), F32)],
        [VMEM] * 3 + [SMEM] * 2 + [VMEM] * len(backs),
        6 * rows * count,
        near, far, sib_got, near_list, near_count, *backs,
    )
    return out


def solution(mesh):
    in_specs = (
        P("leaf", None),
        P("leaf", None),
        P("leaf", None),
        P("leaf", None, None, None),
        P("leaf", None, None, None),
        P("leaf", None),
        P("leaf"),
    )
    out_specs = P("leaf", None)
    return jax.shard_map(shards, mesh=mesh, in_specs=in_specs, out_specs=out_specs, check_vma=False)
```

```python
import functools

import jax
import jax.numpy as jnp
from jax import lax
from jax.experimental import pallas as pl
from jax.experimental.pallas import tpu as pltpu
from jax.sharding import PartitionSpec as P

BF16 = jnp.bfloat16
F32 = jnp.float32
VMEM = pl.BlockSpec(memory_space=pltpu.VMEM)
SMEM = pl.BlockSpec(memory_space=pltpu.SMEM)
HBM = pl.BlockSpec(memory_space=pltpu.HBM)
ANY = pl.BlockSpec(memory_space=pl.ANY)
NN = (((1,), (0,)), ((), ()))
NT = (((1,), (1,)), ((), ()))
TN = (((0,), (0,)), ((), ()))
FLAG_ROWS = 16
LIMIT = 16 << 20
LOAD_LIMIT = 54800000


def dot(a, b, dims):
    return lax.dot_general(a, b, dims, preferred_element_type=F32)


def halves(a):
    high = a.astype(BF16)
    return high, (a - high.astype(F32)).astype(BF16)


def dot_wide(a, b, dims):
    a_high, a_low = halves(a)
    b_high, b_low = halves(b)
    return dot(a_high, b_high, dims) + (dot(a_high, b_low, dims) + dot(a_low, b_high, dims))


def dot_half(a16, b, dims):
    b_high, b_low = halves(b)
    return dot(a16, b_high, dims) + dot(a16, b_low, dims)


def member(list_ref, count_ref, offset):
    index = lax.axis_index("leaf")
    found = jnp.float32(0.0)
    for slot in range(list_ref.shape[1]):
        hit = (list_ref[0, slot] == index + offset) & (slot < count_ref[0])
        found = jnp.where(hit, jnp.float32(1.0), found)
    return found


def call(kernel, outs, specs, flops, *args, scratch=(), limit=LIMIT):
    out_bytes = sum(o.size * o.dtype.itemsize for o in outs)
    in_bytes = sum(a.size * a.dtype.itemsize for a in args)
    return pl.pallas_call(
        kernel,
        out_shape=outs,
        in_specs=specs,
        out_specs=[VMEM] * len(outs),
        scratch_shapes=list(scratch),
        compiler_params=pltpu.CompilerParams(vmem_limit_bytes=limit),
        cost_estimate=pl.CostEstimate(flops=flops, bytes_accessed=in_bytes + out_bytes, transcendentals=0),
    )(*args)


def load_kernel(f_hbm, x_hbm, bases_hbm, transfers_hbm, far_ref, x_ref, bases_ref, transfer_ref, sems):
    size = far_ref.shape[0]
    width = f_hbm.shape[1]
    copies = [
        pltpu.make_async_copy(x_hbm, x_ref, sems.at[0]),
        pltpu.make_async_copy(f_hbm.at[:size], far_ref.at[:, :width], sems.at[1]),
        pltpu.make_async_copy(bases_hbm, bases_ref, sems.at[2]),
        pltpu.make_async_copy(transfers_hbm.at[0, 0], transfer_ref, sems.at[3]),
    ]
    for copy in copies:
        copy.start()
    copies[0].wait()
    far_ref[:, width:] = x_ref[:size].astype(BF16)
    for copy in copies[1:]:
        copy.wait()


def leaf_kernel(c1, bases_ref, x_ref, transfer_ref, message_ref):
    x = x_ref[...]
    rows, probes = x.shape
    skeleton = dot_wide(x, bases_ref[...], TN)
    message_ref[:probes] = skeleton
    message_ref[probes : 2 * probes] = c1 * dot_wide(skeleton, transfer_ref[...], NN)
    message_ref[2 * probes :, :probes] = x[: rows // 2]
    message_ref[2 * probes :, probes:] = x[rows // 2 :]


def pack_kernel(sizes, first, f_ref, x_ref, after_ref, list_ref, count_ref, *far_refs):
    width = f_ref.shape[1]
    probes = x_ref.shape[1]
    for size, far_ref in zip(sizes, far_refs):
        far_ref[:size, :width] = f_ref[first : first + size]
        far_ref[:size, width:] = x_ref[first : first + size].astype(BF16)
        first += size
    flags = [jnp.full((FLAG_ROWS, probes), member(list_ref, count_ref, offset), F32) for offset in (-2, -1)]
    flags.append(jnp.zeros((FLAG_ROWS, width - probes), F32))
    far_refs[0][sizes[0] :] = jnp.concatenate(flags, axis=1).astype(BF16)


def up_kernel(level, factor, own_ref, got_ref, transfer_ref, message_ref, next_ref):
    probes = next_ref.shape[0]
    own = own_ref[probes : 2 * probes] if own_ref.shape[0] > probes else own_ref[...]
    skeleton = own + got_ref[probes : 2 * probes].astype(F32)
    message_ref[:probes] = skeleton.astype(message_ref.dtype)
    if factor is not None:
        moved = factor * dot_wide(skeleton, transfer_ref[0, level], NN)
        message_ref[probes:] = moved.astype(message_ref.dtype)
        next_ref[...] = moved
    else:
        next_ref[...] = skeleton


def down_kernel(scale_g, factors, got0_ref, *refs):
    depth = len(factors)
    gots = [got0_ref, *refs[:depth]]
    coupling_ref, transfer_ref, bases_ref, out_ref = refs[depth:]
    probes = out_ref.shape[1]
    expansion = None
    for level in range(depth, -1, -1):
        got = gots[level][:probes]
        wide = dot_wide if got.dtype == F32 else dot_half
        update = scale_g * wide(got, coupling_ref[0, level], NT)
        if level < depth:
            update = update + factors[level] * dot_wide(expansion, transfer_ref[0, level], NT)
        expansion = update
    out_ref[...] = dot_wide(bases_ref[...], expansion, NT)


def tile(rows_a, rows_b, scale):
    gram = dot(rows_a, rows_b, NT)
    return halves(gram * gram * scale)


def self_kernel(scale, f_ref, x_ref, out_ref):
    high, low = tile(f_ref[...], f_ref[...], scale)
    x_high, x_low = halves(x_ref[...])
    out_ref[...] = dot(high, x_high, NN) + (dot(high, x_low, NN) + dot(low, x_high, NN))


def times(parts, x16):
    return dot(parts[0], x16, NN) + dot(parts[1], x16, NN)


def times_back(parts, xt16):
    return (dot(xt16, parts[0], NN) + dot(xt16, parts[1], NN)).T


def pair_kernel(scale, f_ref, g_ref, near_ref, x_ref, got_ref, list_ref, count_ref, out_ref, sib_ref, xt_ref, xst_ref):
    odd = lax.rem(lax.axis_index("leaf"), 2) == 1
    rows, probes = near_ref.shape
    xt_ref[...] = x_ref[...].T.astype(BF16)
    for half in range(2):
        part = got_ref[2 * probes :, half * probes : (half + 1) * probes]
        xst_ref[:, half * (rows // 2) : (half + 1) * (rows // 2)] = part.T.astype(BF16)

    @pl.when(odd)
    def _():
        parts = tile(g_ref[...], f_ref[...], scale)
        sib_ref[...] = times(parts, x_ref[...].astype(BF16))
        flag = member(list_ref, count_ref, -1)
        out_ref[...] = near_ref[...] + flag * times_back(parts, xst_ref[...])

    @pl.when(jnp.logical_not(odd))
    def _():
        out_ref[...] = near_ref[...]
        sib_ref[...] = jnp.zeros_like(sib_ref)


def chunk_kernel(scale, size, head, stage, f_ref, g_ref, h_ref, near_ref, sib_in_ref, xt_ref, xst_ref, list_ref, count_ref, *refs):
    even = lax.rem(lax.axis_index("leaf"), 2) == 0
    width = f_ref.shape[1]
    probes = near_ref.shape[1]
    h = h_ref[:size, :width]
    xh = h_ref[:size, width:]
    extra = 0
    if stage:
        flags_ref = refs[0]
        extra = 1
        at = flags_ref.shape[0] - FLAG_ROWS
        flag2 = flags_ref[at : at + 1, :probes].astype(F32)
        flag1 = flags_ref[at : at + 1, probes : 2 * probes].astype(F32)
    if stage == 1:
        far_head, near_head = refs[1:3]
        extra = 3
    out_ref, sib_ref, *back_refs = refs[extra:]
    parts = tile(f_ref[...], h, scale)
    out_ref[...] = near_ref[...] + member(list_ref, count_ref, 2) * times(parts, xh)
    back = times_back(parts, xt_ref[...])
    if stage == 0:
        back_refs[0][...] = back
    else:
        back = flag2 * back
    if stage == 1:
        back_refs[0][:head] = (flag2 * far_head[...] + flag1 * near_head[...]).astype(BF16)

    @pl.when(even)
    def _():
        cross = tile(g_ref[...], h, scale)
        sib_ref[...] = (sib_in_ref[...] + times(cross, xh)).astype(sib_ref.dtype)
        cross_back = times_back(cross, xst_ref[...])
        if stage == 0:
            back_refs[1][...] = cross_back
        else:
            back_refs[0][head:] = (back + flag1 * cross_back).astype(BF16)

    @pl.when(jnp.logical_not(even))
    def _():
        sib_ref[...] = sib_in_ref[...].astype(sib_ref.dtype)
        if stage == 0:
            back_refs[1][...] = jnp.zeros_like(back_refs[1])
        else:
            back_refs[0][head:] = back.astype(BF16)


def final_kernel(near_ref, far_ref, sib_ref, list_ref, count_ref, *refs):
    out_ref = refs[-1]
    flag = member(list_ref, count_ref, 1)
    at = 0
    for back_ref in refs[:-1]:
        rows = slice(at, at + back_ref.shape[0])
        out_ref[rows] = near_ref[rows] + far_ref[rows] + flag * sib_ref[rows].astype(F32) + back_ref[...].astype(F32)
        at += back_ref.shape[0]


def moved(array, by):
    peers = lax.axis_size("leaf")
    return lax.ppermute(array, "leaf", [(i, i + by) for i in range(peers) if 0 <= i + by < peers])


def partner(array, level):
    return lax.ppermute(array, "leaf", [(i, i ^ 1 << level) for i in range(lax.axis_size("leaf"))])


def body(features, probes, bases, transfers, couplings, near_list, near_count):
    rows, width = features.shape
    count = probes.shape[1]
    rank = bases.shape[1]
    depth = transfers.shape[1]
    scale = 1.0 / (rows * width)
    scale_g = (3.0 / rank) ** 0.5
    factors = [scale_g * 2.0 ** (-0.5 * (level + 1)) for level in range(depth)]
    shape = jax.ShapeDtypeStruct
    sizes = [rows // 4, rows // 2, rows // 4]

    sib_features = partner(features, 0)
    far0_out, x, bases_v, transfer0 = call(
        load_kernel,
        [
            shape((sizes[0], width + count), BF16),
            shape((rows, count), F32),
            shape((rows, rank), F32),
            shape((rank, rank), F32),
        ],
        [HBM] * 4,
        1000,
        features, probes, bases, transfers,
        scratch=[pltpu.SemaphoreType.DMA((4,))],
        limit=LOAD_LIMIT,
    )
    far = [moved(far0_out, -2)]
    (message,) = call(
        functools.partial(leaf_kernel, factors[0]),
        [shape((2 * count + rows // 2, rank), F32)],
        [VMEM] * 3,
        6 * rows * rank * count,
        bases_v, x, transfer0,
    )
    gots = [partner(message, 0)]
    own = message
    for level in range(1, depth + 1):
        last = level == depth
        outs = [shape((count if last else 2 * count, rank), BF16), shape((count, rank), F32)]
        message, own = call(
            functools.partial(up_kernel, level, None if last else factors[level]),
            outs,
            [VMEM] * 3,
            6 * rank * rank * count,
            own, gots[-1], transfers,
        )
        gots.append(partner(message, level))
        if level == 1:
            packed = call(
                functools.partial(pack_kernel, sizes[1:], sizes[0]),
                [shape((size + (0 if i else FLAG_ROWS), width + count), BF16) for i, size in enumerate(sizes[1:])],
                [VMEM, VMEM, ANY, SMEM, SMEM],
                1000,
                features, x, message, near_list, near_count,
            )
            far += [moved(part, -2) for part in packed]

    tile_flops = 2 * rows * rows * (width + 4 * count)
    (near,) = call(
        functools.partial(self_kernel, scale),
        [shape((rows, count), F32)],
        [VMEM, VMEM],
        tile_flops,
        features, x,
    )
    near, sib, xt, xst = call(
        functools.partial(pair_kernel, scale),
        [shape((rows, count), F32)] * 2 + [shape((count, rows), BF16)] * 2,
        [VMEM] * 5 + [SMEM] * 2,
        tile_flops,
        features, sib_features, near, x, gots[0], near_list, near_count,
    )
    backs = []
    heads = []
    for stage, (size, part) in enumerate(zip(sizes, far)):
        head = sizes[0] if stage == 1 else 0
        more = [[], [far[1], *heads], [far[1]]][stage]
        back_shapes = [shape((size, count), F32)] * 2 if stage == 0 else [shape((head + size, count), BF16)]
        near, sib, *heads = call(
            functools.partial(chunk_kernel, scale, size, head, stage),
            [shape((rows, count), F32), shape((rows, count), BF16 if stage == 2 else F32), *back_shapes],
            [VMEM] * 7 + [SMEM] * 2 + [VMEM] * len(more),
            tile_flops * 2 * size // rows,
            features, sib_features, part, near, sib, xt, xst, near_list, near_count, *more,
        )
        if stage:
            backs.append(moved(heads[0], 2))
    sib_got = partner(sib, 0)
    (far_sum,) = call(
        functools.partial(down_kernel, scale_g, factors),
        [shape((rows, count), F32)],
        [VMEM] * (depth + 4),
        6 * count * rank * (rank * (2 * depth + 1) + rows),
        *gots, couplings, transfers, bases_v,
    )
    (out,) = call(
        final_kernel,
        [shape((rows, count), F32)],
        [VMEM] * 3 + [SMEM] * 2 + [VMEM] * len(backs),
        6 * rows * count,
        near, far_sum, sib_got, near_list, near_count, *backs,
    )
    return out


def solution(mesh):
    in_specs = (
        P("leaf", None),
        P("leaf", None),
        P("leaf", None),
        P("leaf", None, None, None),
        P("leaf", None, None, None),
        P("leaf", None),
        P("leaf"),
    )
    out_specs = P("leaf", None)
    return jax.shard_map(body, mesh=mesh, in_specs=in_specs, out_specs=out_specs, check_vma=False)
```

```python
import functools

import jax
import jax.numpy as jnp
from jax import lax
from jax.experimental import pallas as pl
from jax.experimental.pallas import tpu as pltpu
from jax.sharding import PartitionSpec as P

BF16 = jnp.bfloat16
F32 = jnp.float32
VMEM = pl.BlockSpec(memory_space=pltpu.VMEM)
SMEM = pl.BlockSpec(memory_space=pltpu.SMEM)
HBM = pl.BlockSpec(memory_space=pltpu.HBM)
ANY = pl.BlockSpec(memory_space=pl.ANY)
NN = (((1,), (0,)), ((), ()))
NT = (((1,), (1,)), ((), ()))
TN = (((0,), (0,)), ((), ()))
FLAG_ROWS = 16
LIMIT = 16 << 20
LOAD_LIMIT = 55500000
SHARED = ((), ((0, 1),), ((0, 1), (1, 0)), ((0, 1), (1, 0), (2, 1)))


def dot(a, b, dims):
    return lax.dot_general(a, b, dims, preferred_element_type=F32)


def halves(a):
    high = a.astype(BF16)
    return high, (a - high.astype(F32)).astype(BF16)


def dot_wide(a, b, dims):
    a_high, a_low = halves(a)
    b_high, b_low = halves(b)
    return dot(a_high, b_high, dims) + (dot(a_high, b_low, dims) + dot(a_low, b_high, dims))


def dot_half(a16, b, dims):
    b_high, b_low = halves(b)
    return dot(a16, b_high, dims) + dot(a16, b_low, dims)


def member(list_ref, count_ref, offset):
    index = lax.axis_index("leaf")
    found = jnp.float32(0.0)
    for slot in range(list_ref.shape[1]):
        hit = (list_ref[0, slot] == index + offset) & (slot < count_ref[0])
        found = jnp.where(hit, jnp.float32(1.0), found)
    return found


def call(kernel, outs, specs, flops, *args, scratch=(), limit=LIMIT):
    out_bytes = sum(o.size * o.dtype.itemsize for o in outs)
    in_bytes = sum(a.size * a.dtype.itemsize for a in args)
    return pl.pallas_call(
        kernel,
        out_shape=outs,
        in_specs=specs,
        out_specs=[VMEM] * len(outs),
        scratch_shapes=list(scratch),
        compiler_params=pltpu.CompilerParams(vmem_limit_bytes=limit),
        cost_estimate=pl.CostEstimate(flops=flops, bytes_accessed=in_bytes + out_bytes, transcendentals=0),
    )(*args)


def leaf_kernel(c1, bases_hbm, x_hbm, transfers_hbm, message_ref, bases_ref, x_ref, transfer_ref, sems):
    copies = [
        pltpu.make_async_copy(x_hbm, x_ref, sems.at[0]),
        pltpu.make_async_copy(bases_hbm, bases_ref, sems.at[1]),
        pltpu.make_async_copy(transfers_hbm.at[0, 0], transfer_ref, sems.at[2]),
    ]
    for copy in copies:
        copy.start()
    for copy in copies:
        copy.wait()
    x = x_ref[...]
    rows, probes = x.shape
    skeleton = dot_wide(x, bases_ref[...], TN)
    message_ref[:probes] = skeleton
    message_ref[probes : 2 * probes] = c1 * dot_wide(skeleton, transfer_ref[...], NN)
    message_ref[2 * probes :, :probes] = x[: rows // 2]
    message_ref[2 * probes :, probes:] = x[rows // 2 :]


def pack_kernel(sizes, f_ref, x_ref, list_ref, count_ref, *far_refs):
    width = f_ref.shape[1]
    probes = x_ref.shape[1]
    first = 0
    for size, far_ref in zip(sizes, far_refs):
        far_ref[:size, :width] = f_ref[first : first + size]
        far_ref[:size, width:] = x_ref[first : first + size].astype(BF16)
        first += size
    flags = [jnp.full((FLAG_ROWS, probes), member(list_ref, count_ref, offset), F32) for offset in (-2, -1)]
    flags.append(jnp.zeros((FLAG_ROWS, width - probes), F32))
    far_refs[0][sizes[0] :] = jnp.concatenate(flags, axis=1).astype(BF16)


def up_kernel(level, factor, own_ref, got_ref, transfer_ref, message_ref, next_ref):
    probes = next_ref.shape[0]
    own = own_ref[probes : 2 * probes] if own_ref.shape[0] > probes else own_ref[...]
    skeleton = own + got_ref[probes : 2 * probes].astype(F32)
    message_ref[:probes] = skeleton.astype(message_ref.dtype)
    moved = factor * dot_wide(skeleton, transfer_ref[0, level], NN)
    if message_ref.shape[0] > probes:
        message_ref[probes:] = moved.astype(message_ref.dtype)
    next_ref[...] = moved.astype(next_ref.dtype)


def bit_of(level):
    return lax.rem(lax.axis_index("leaf") >> level, 2)


def descend(scale_g, factor, got, coupling, transfer, above):
    wide = dot_wide if got.dtype == F32 else dot_half
    update = scale_g * wide(got, coupling, NT)
    return update if above is None else update + factor * dot_wide(above, transfer, NT)


def top_kernel(scale_g, factor, coupling_ref, transfer_ref, got_ref, term_ref, other_ref, own_ref, message_ref):
    depth = transfer_ref.shape[1]
    sibling = term_ref[...].astype(F32) + other_ref[...].astype(F32)
    root = descend(scale_g, None, sibling, coupling_ref[0, depth], None, None)
    out = descend(scale_g, factor, got_ref[...], coupling_ref[0, depth - 1], transfer_ref[0, depth - 1], root)
    own_ref[...] = out
    message_ref[...] = out.astype(BF16)


def middle_kernel(scale_g, factor, level, coupling_ref, transfer_ref, got_ref, above_ref, sent_ref, own_ref, message_ref):
    probes = own_ref.shape[0]
    above = jnp.where(bit_of(level) == 1, above_ref[...], sent_ref[...].astype(F32))
    out = descend(scale_g, factor, got_ref[:probes], coupling_ref[0, level], transfer_ref[0, level], above)
    own_ref[...] = out
    message_ref[...] = out.astype(BF16)


def node_kernel(scale_g, factor, level, coupling_ref, transfer_ref, got_ref, above_ref, sent_ref, own_ref):
    probes = own_ref.shape[0]
    above = jnp.where(bit_of(level) == 0, above_ref[...], sent_ref[...].astype(F32))
    own_ref[...] = descend(scale_g, factor, got_ref[:probes], coupling_ref[0, level], transfer_ref[0, level], above)


def down_kernel(scale_g, factor, coupling_ref, transfer_ref, bases_ref, got_ref, above_ref, sent_ref, out_ref):
    probes = out_ref.shape[1]
    above = jnp.where(bit_of(0) == 1, above_ref[...], sent_ref[...])
    expansion = descend(scale_g, factor, got_ref[:probes], coupling_ref[0, 0], transfer_ref[0, 0], above)
    out_ref[...] = dot_wide(bases_ref[...], expansion, NT)


def tile(rows_a, rows_b, scale):
    gram = dot(rows_a, rows_b, NT)
    return halves(gram * gram * scale)


def self_kernel(scale, f_ref, x_ref, out_ref):
    high, low = tile(f_ref[...], f_ref[...], scale)
    x_high, x_low = halves(x_ref[...])
    out_ref[...] = dot(high, x_high, NN) + (dot(high, x_low, NN) + dot(low, x_high, NN))


def times(parts, x16):
    return dot(parts[0], x16, NN) + dot(parts[1], x16, NN)


def times_back(parts, xt16):
    return (dot(xt16, parts[0], NN) + dot(xt16, parts[1], NN)).T


def pair_kernel(scale, f_ref, g_ref, near_ref, x_ref, got_ref, list_ref, count_ref, out_ref, sib_ref, xt_ref, xst_ref):
    odd = lax.rem(lax.axis_index("leaf"), 2) == 1
    rows, probes = near_ref.shape
    xt_ref[...] = x_ref[...].T.astype(BF16)
    for half in range(2):
        part = got_ref[2 * probes :, half * probes : (half + 1) * probes]
        xst_ref[:, half * (rows // 2) : (half + 1) * (rows // 2)] = part.T.astype(BF16)

    @pl.when(odd)
    def _():
        parts = tile(g_ref[...], f_ref[...], scale)
        sib_ref[...] = times(parts, x_ref[...].astype(BF16))
        flag = member(list_ref, count_ref, -1)
        out_ref[...] = near_ref[...] + flag * times_back(parts, xst_ref[...])

    @pl.when(jnp.logical_not(odd))
    def _():
        out_ref[...] = near_ref[...]
        sib_ref[...] = jnp.zeros_like(sib_ref)


def chunk_kernel(scale, size, f_ref, g_ref, h_ref, flags_ref, near_ref, sib_in_ref, xt_ref, xst_ref, list_ref, count_ref, out_ref, sib_ref, back_ref):
    even = lax.rem(lax.axis_index("leaf"), 2) == 0
    width = f_ref.shape[1]
    probes = near_ref.shape[1]
    h = h_ref[:size, :width]
    xh = h_ref[:size, width:]
    at = flags_ref.shape[0] - FLAG_ROWS
    flag2 = flags_ref[at : at + 1, :probes].astype(F32)
    flag1 = flags_ref[at : at + 1, probes : 2 * probes].astype(F32)
    parts = tile(f_ref[...], h, scale)
    out_ref[...] = near_ref[...] + member(list_ref, count_ref, 2) * times(parts, xh)
    back = flag2 * times_back(parts, xt_ref[...])

    @pl.when(even)
    def _():
        cross = tile(g_ref[...], h, scale)
        sib_ref[...] = (sib_in_ref[...] + times(cross, xh)).astype(sib_ref.dtype)
        back_ref[...] = (back + flag1 * times_back(cross, xst_ref[...])).astype(BF16)

    @pl.when(jnp.logical_not(even))
    def _():
        sib_ref[...] = sib_in_ref[...].astype(sib_ref.dtype)
        back_ref[...] = back.astype(BF16)


def final_kernel(near_ref, far_ref, sib_ref, list_ref, count_ref, *refs):
    out_ref = refs[-1]
    flag = member(list_ref, count_ref, 1)
    at = 0
    for back_ref in refs[:-1]:
        rows = slice(at, at + back_ref.shape[0])
        out_ref[rows] = near_ref[rows] + far_ref[rows] + flag * sib_ref[rows].astype(F32) + back_ref[...].astype(F32)
        at += back_ref.shape[0]


def moved(array, by):
    peers = lax.axis_size("leaf")
    return lax.ppermute(array, "leaf", [(i, i + by) for i in range(peers) if 0 <= i + by < peers])


def across(array, distance, bits=()):
    senders = [i for i in range(lax.axis_size("leaf")) if all(i >> at & 1 == bit for at, bit in bits)]
    return lax.ppermute(array, "leaf", [(i, i ^ distance) for i in senders])


def partner(array, level, bits=()):
    return across(array, 1 << level, bits)


def body(features, probes, bases, transfers, couplings, near_list, near_count):
    rows, width = features.shape
    count = probes.shape[1]
    rank = bases.shape[1]
    depth = transfers.shape[1]
    scale = 1.0 / (rows * width)
    scale_g = (3.0 / rank) ** 0.5
    factors = [scale_g * 2.0 ** (-0.5 * (level + 1)) for level in range(depth)]
    shape = jax.ShapeDtypeStruct
    sizes = [rows // 2, rows // 2]

    sib_features = partner(features, 0)
    (message,) = call(
        functools.partial(leaf_kernel, factors[0]),
        [shape((2 * count + rows // 2, rank), F32)],
        [HBM] * 3,
        6 * rows * rank * count,
        bases, probes, transfers,
        scratch=[
            pltpu.VMEM((rows, rank), F32),
            pltpu.VMEM((rows, count), F32),
            pltpu.VMEM((rank, rank), F32),
            pltpu.SemaphoreType.DMA((3,)),
        ],
        limit=LOAD_LIMIT,
    )
    gots = [partner(message, 0)]
    packed = call(
        functools.partial(pack_kernel, sizes),
        [shape((size + (0 if i else FLAG_ROWS), width + count), BF16) for i, size in enumerate(sizes)],
        [VMEM, VMEM, SMEM, SMEM],
        1000,
        features, probes, near_list, near_count,
    )
    far = [moved(part, -2) for part in packed]
    own = [message]
    top = depth - 1
    for level in range(1, top + 1):
        message, *own = call(
            functools.partial(up_kernel, level, factors[level]),
            [shape((2 * count, rank), BF16), shape((count, rank), F32)] if level < top else [shape((count, rank), BF16)] * 2,
            [VMEM] * 3,
            6 * rank * rank * count,
            *own, gots[-1], transfers,
        )
        if level < top:
            gots.append(partner(message, level, SHARED[level]))
    gots.append(partner(message, top, SHARED[top]))
    terms = [across(own[0], (1 << top + 1) + extra, SHARED[top]) for extra in (0, 1 << top)]

    tile_flops = 2 * rows * rows * (width + 4 * count)
    (near,) = call(
        functools.partial(self_kernel, scale),
        [shape((rows, count), F32)],
        [VMEM, VMEM],
        tile_flops,
        features, probes,
    )
    near, sib, xt, xst = call(
        functools.partial(pair_kernel, scale),
        [shape((rows, count), F32)] * 2 + [shape((count, rows), BF16)] * 2,
        [VMEM] * 5 + [SMEM] * 2,
        tile_flops,
        features, sib_features, near, probes, gots[0], near_list, near_count,
    )
    backs = []
    for stage, (size, part) in enumerate(zip(sizes, far)):
        last = stage == len(sizes) - 1
        near, sib, back = call(
            functools.partial(chunk_kernel, scale, size),
            [shape((rows, count), F32), shape((rows, count), BF16 if last else F32), shape((size, count), BF16)],
            [VMEM] * 8 + [SMEM] * 2,
            tile_flops * 2 * size // rows,
            features, sib_features, part, far[0], near, sib, xt, xst, near_list, near_count,
        )
        backs.append(moved(back, 2))
    sib_got = partner(sib, 0)
    product_flops = 6 * count * rank * rank
    e3, e3_message = call(
        functools.partial(top_kernel, scale_g, factors[top]),
        [shape((count, rank), F32), shape((count, rank), BF16)],
        [VMEM] * 5,
        3 * product_flops,
        couplings, transfers, gots[top], *terms,
    )
    e3_sent = partner(e3_message, 2, SHARED[3])
    e2, e2_message = call(
        functools.partial(middle_kernel, scale_g, factors[2], 2),
        [shape((count, rank), F32), shape((count, rank), BF16)],
        [VMEM] * 5,
        2 * product_flops,
        couplings, transfers, gots[2], e3, e3_sent,
    )
    e2_sent = partner(e2_message, 1, SHARED[2])
    (e1,) = call(
        functools.partial(node_kernel, scale_g, factors[1], 1),
        [shape((count, rank), F32)],
        [VMEM] * 5,
        2 * product_flops,
        couplings, transfers, gots[1], e2, e2_sent,
    )
    e1_sent = partner(e1, 0, SHARED[1])
    (far_sum,) = call(
        functools.partial(down_kernel, scale_g, factors[0]),
        [shape((rows, count), F32)],
        [VMEM] * 6,
        2 * product_flops + 6 * rows * rank * count,
        couplings, transfers, bases, gots[0], e1, e1_sent,
    )
    (out,) = call(
        final_kernel,
        [shape((rows, count), F32)],
        [VMEM] * 3 + [SMEM] * 2 + [VMEM] * len(backs),
        6 * rows * count,
        near, far_sum, sib_got, near_list, near_count, *backs,
    )
    return out


def solution(mesh):
    in_specs = (
        P("leaf", None),
        P("leaf", None),
        P("leaf", None),
        P("leaf", None, None, None),
        P("leaf", None, None, None),
        P("leaf", None),
        P("leaf"),
    )
    out_specs = P("leaf", None)
    return jax.shard_map(body, mesh=mesh, in_specs=in_specs, out_specs=out_specs, check_vma=False)
```

```python
import functools

import jax
import jax.numpy as jnp
from jax import lax
from jax.experimental import pallas as pl
from jax.experimental.pallas import tpu as pltpu
from jax.sharding import PartitionSpec as P

BF16 = jnp.bfloat16
F32 = jnp.float32
VMEM = pl.BlockSpec(memory_space=pltpu.VMEM)
SMEM = pl.BlockSpec(memory_space=pltpu.SMEM)
HBM = pl.BlockSpec(memory_space=pltpu.HBM)
ANY = pl.BlockSpec(memory_space=pl.ANY)
NN = (((1,), (0,)), ((), ()))
NT = (((1,), (1,)), ((), ()))
TN = (((0,), (0,)), ((), ()))
FLAG_ROWS = 8
LIMIT = 16 << 20
LOAD_LIMIT = 55500000
SHARED = ((), ((0, 1),), ((0, 1), (1, 0)), ((0, 1), (1, 0), (2, 1)))


def dot(a, b, dims):
    return lax.dot_general(a, b, dims, preferred_element_type=F32)


def halves(a):
    high = a.astype(BF16)
    return high, (a - high.astype(F32)).astype(BF16)


def dot_wide(a, b, dims):
    a_high, a_low = halves(a)
    b_high, b_low = halves(b)
    return dot(a_high, b_high, dims) + (dot(a_high, b_low, dims) + dot(a_low, b_high, dims))


def dot_half(a16, b, dims):
    b_high, b_low = halves(b)
    return dot(a16, b_high, dims) + dot(a16, b_low, dims)


def member(list_ref, count_ref, offset):
    index = lax.axis_index("leaf")
    found = jnp.float32(0.0)
    for slot in range(list_ref.shape[1]):
        hit = (list_ref[0, slot] == index + offset) & (slot < count_ref[0])
        found = jnp.where(hit, jnp.float32(1.0), found)
    return found


def call(kernel, outs, specs, flops, *args, scratch=(), limit=LIMIT):
    out_bytes = sum(o.size * o.dtype.itemsize for o in outs)
    in_bytes = sum(a.size * a.dtype.itemsize for a in args)
    return pl.pallas_call(
        kernel,
        out_shape=outs,
        in_specs=specs,
        out_specs=[VMEM] * len(outs),
        scratch_shapes=list(scratch),
        compiler_params=pltpu.CompilerParams(vmem_limit_bytes=limit),
        cost_estimate=pl.CostEstimate(flops=flops, bytes_accessed=in_bytes + out_bytes, transcendentals=0),
    )(*args)


def leaf_kernel(c1, bases_hbm, x_hbm, transfers_hbm, message_ref, bases_ref, x_ref, transfer_ref, sems):
    copies = [
        pltpu.make_async_copy(x_hbm, x_ref, sems.at[0]),
        pltpu.make_async_copy(bases_hbm, bases_ref, sems.at[1]),
        pltpu.make_async_copy(transfers_hbm.at[0, 0], transfer_ref, sems.at[2]),
    ]
    for copy in copies:
        copy.start()
    for copy in copies:
        copy.wait()
    x = x_ref[...]
    rows, probes = x.shape
    skeleton = dot_wide(x, bases_ref[...], TN)
    message_ref[:probes] = skeleton
    message_ref[probes : 2 * probes] = c1 * dot_wide(skeleton, transfer_ref[...], NN)
    message_ref[2 * probes :, :probes] = x[: rows // 2]
    message_ref[2 * probes :, probes:] = x[rows // 2 :]


def pack_kernel(first, f_ref, x_ref, list_ref, count_ref, far_ref):
    rows, width = f_ref.shape
    probes = x_ref.shape[1]
    size = min(far_ref.shape[0], rows - first)
    far_ref[:size, :width] = f_ref[first : first + size]
    far_ref[:size, width:] = x_ref[first : first + size].astype(BF16)
    if far_ref.shape[0] > size:
        flags = [jnp.full((FLAG_ROWS, probes), member(list_ref, count_ref, offset), F32) for offset in (-2, -1)]
        flags.append(jnp.zeros((FLAG_ROWS, width - probes), F32))
        far_ref[size:] = jnp.concatenate(flags, axis=1).astype(BF16)


def up_kernel(level, factor, own_ref, got_ref, transfer_ref, message_ref, *next_refs):
    probes = message_ref.shape[0] if factor is None else message_ref.shape[0] // 2
    own = own_ref[probes : 2 * probes] if own_ref.shape[0] > probes else own_ref[...]
    skeleton = own + got_ref[probes : 2 * probes].astype(F32)
    message_ref[:probes] = skeleton.astype(message_ref.dtype)
    if factor is not None:
        moved = factor * dot_wide(skeleton, transfer_ref[0, level], NN)
        message_ref[probes:] = moved.astype(message_ref.dtype)
        next_refs[0][...] = moved


def bit_of(level):
    return lax.rem(lax.axis_index("leaf") >> level, 2)


def descend(scale_g, factor, got, coupling, transfer, above):
    wide = dot_wide if got.dtype == F32 else dot_half
    update = scale_g * wide(got, coupling, NT)
    return update if above is None else update + factor * dot_wide(above, transfer, NT)


def top_kernel(scale_g, factor, coupling_ref, transfer_ref, got_ref, root_ref, own_ref, message_ref):
    depth = transfer_ref.shape[1]
    probes = own_ref.shape[0]
    root = descend(scale_g, None, root_ref[...], coupling_ref[0, depth], None, None)
    out = descend(scale_g, factor, got_ref[:probes], coupling_ref[0, depth - 1], transfer_ref[0, depth - 1], root)
    own_ref[...] = out
    message_ref[...] = out.astype(BF16)


def middle_kernel(scale_g, factor, level, coupling_ref, transfer_ref, got_ref, above_ref, sent_ref, own_ref, message_ref):
    probes = own_ref.shape[0]
    above = jnp.where(bit_of(level) == 1, above_ref[...], sent_ref[...].astype(F32))
    out = descend(scale_g, factor, got_ref[:probes], coupling_ref[0, level], transfer_ref[0, level], above)
    own_ref[...] = out
    message_ref[...] = out.astype(BF16)


def node_kernel(scale_g, factor, level, coupling_ref, transfer_ref, got_ref, above_ref, sent_ref, sib_ref, own_ref, message_ref):
    probes, rank = own_ref.shape
    rows = sib_ref.shape[0]
    above = jnp.where(bit_of(level) == 0, above_ref[...], sent_ref[...].astype(F32))
    out = descend(scale_g, factor, got_ref[:probes], coupling_ref[0, level], transfer_ref[0, level], above)
    own_ref[...] = out
    message_ref[:rows] = sib_ref[...]
    for part in range(rank // probes):
        message_ref[rows + part * probes : rows + (part + 1) * probes] = out[:, part * probes : (part + 1) * probes]


def down_kernel(scale_g, factor, coupling_ref, transfer_ref, bases_ref, got_ref, above_ref, sent_ref, out_ref):
    rows, probes = out_ref.shape
    rank = bases_ref.shape[1]
    sent = [sent_ref[rows + part * probes : rows + (part + 1) * probes] for part in range(rank // probes)]
    above = jnp.where(bit_of(0) == 1, above_ref[...], jnp.concatenate(sent, axis=1))
    expansion = descend(scale_g, factor, got_ref[:probes], coupling_ref[0, 0], transfer_ref[0, 0], above)
    out_ref[...] = dot_wide(bases_ref[...], expansion, NT)


def tile(rows_a, rows_b, scale):
    gram = dot(rows_a, rows_b, NT)
    return halves(gram * gram * scale)


def self_kernel(scale, f_ref, x_ref, out_ref):
    high, low = tile(f_ref[...], f_ref[...], scale)
    x_high, x_low = halves(x_ref[...])
    out_ref[...] = dot(high, x_high, NN) + (dot(high, x_low, NN) + dot(low, x_high, NN))


def times(parts, x16):
    return dot(parts[0], x16, NN) + dot(parts[1], x16, NN)


def times_back(parts, xt16):
    return (dot(xt16, parts[0], NN) + dot(xt16, parts[1], NN)).T


def pair_kernel(scale, f_ref, g_ref, near_ref, x_ref, got_ref, list_ref, count_ref, out_ref, sib_ref, xt_ref, xst_ref):
    odd = lax.rem(lax.axis_index("leaf"), 2) == 1
    rows, probes = near_ref.shape
    xt_ref[...] = x_ref[...].T.astype(BF16)
    for half in range(2):
        part = got_ref[2 * probes :, half * probes : (half + 1) * probes]
        xst_ref[:, half * (rows // 2) : (half + 1) * (rows // 2)] = part.T.astype(BF16)

    @pl.when(odd)
    def _():
        parts = tile(g_ref[...], f_ref[...], scale)
        sib_ref[...] = times(parts, x_ref[...].astype(BF16))
        flag = member(list_ref, count_ref, -1)
        out_ref[...] = near_ref[...] + flag * times_back(parts, xst_ref[...])

    @pl.when(jnp.logical_not(odd))
    def _():
        out_ref[...] = near_ref[...]
        sib_ref[...] = jnp.zeros_like(sib_ref)


def chunk_kernel(scale, size, f_ref, g_ref, even_ref, odd_ref, near_ref, sib_in_ref, xt_ref, xst_ref, list_ref, count_ref, *refs):
    even = lax.rem(lax.axis_index("leaf"), 2) == 0
    width = f_ref.shape[1]
    probes = near_ref.shape[1]
    heads = refs[: len(refs) // 5 * 2]
    out_ref, sib_ref, *back_refs = refs[len(heads) :]
    mine = member(list_ref, count_ref, 2)

    def put(back, cross_back):
        if not heads:
            back_refs[0][...] = back
            back_refs[1][...] = jnp.zeros_like(back) if cross_back is None else cross_back
            return
        head = heads[0].shape[0]
        flag2 = even_ref[size : size + 1, :probes].astype(F32)
        flag1 = even_ref[size : size + 1, probes : 2 * probes].astype(F32)
        back_refs[0][:head] = (flag2 * heads[0][...] + flag1 * heads[1][...]).astype(BF16)
        total = flag2 * back
        back_refs[0][head:] = (total if cross_back is None else total + flag1 * cross_back).astype(BF16)

    @pl.when(even)
    def _():
        h = even_ref[:size, :width]
        xh = even_ref[:size, width:]
        parts = tile(f_ref[...], h, scale)
        out_ref[...] = near_ref[...] + mine * times(parts, xh)
        cross = tile(g_ref[...], h, scale)
        sib_ref[...] = sib_in_ref[...] + times(cross, xh)
        put(times_back(parts, xt_ref[...]), times_back(cross, xst_ref[...]))

    @pl.when(jnp.logical_not(even))
    def _():
        h = odd_ref[:size, :width]
        xh = odd_ref[:size, width:]
        parts = tile(f_ref[...], h, scale)
        out_ref[...] = near_ref[...] + mine * times(parts, xh)
        sib_ref[...] = sib_in_ref[...]
        put(times_back(parts, xt_ref[...]), None)


def final_kernel(near_ref, far_ref, sib_ref, back_ref, list_ref, count_ref, out_ref):
    rows = out_ref.shape[0]
    flag = member(list_ref, count_ref, 1)
    out_ref[...] = near_ref[...] + far_ref[...] + flag * sib_ref[:rows] + back_ref[...].astype(F32)


def sender(index, bits):
    return all(index >> at & 1 == bit for at, bit in bits)


def moved(array, by, bits=()):
    peers = lax.axis_size("leaf")
    pairs = [(i, i + by) for i in range(peers) if 0 <= i + by < peers and sender(i, bits)]
    return lax.ppermute(array, "leaf", pairs)


def across(array, distance, bits=()):
    senders = [i for i in range(lax.axis_size("leaf")) if sender(i, bits)]
    return lax.ppermute(array, "leaf", [(i, i ^ distance) for i in senders])


def partner(array, level, bits=()):
    return across(array, 1 << level, bits)


def body(features, probes, bases, transfers, couplings, near_list, near_count):
    rows, width = features.shape
    count = probes.shape[1]
    rank = bases.shape[1]
    depth = transfers.shape[1]
    scale = 1.0 / (rows * width)
    scale_g = (3.0 / rank) ** 0.5
    factors = [scale_g * 2.0 ** (-0.5 * (level + 1)) for level in range(depth)]
    shape = jax.ShapeDtypeStruct
    sizes = [rows // 2, rows // 2]

    sib_features = partner(features, 0)
    (message,) = call(
        functools.partial(leaf_kernel, factors[0]),
        [shape((2 * count + rows // 2, rank), F32)],
        [HBM] * 3,
        6 * rows * rank * count,
        bases, probes, transfers,
        scratch=[
            pltpu.VMEM((rows, rank), F32),
            pltpu.VMEM((rows, count), F32),
            pltpu.VMEM((rank, rank), F32),
            pltpu.SemaphoreType.DMA((3,)),
        ],
        limit=LOAD_LIMIT,
    )
    gots = [partner(message, 0)]
    packed = []
    for at in range(2):
        packed += call(
            functools.partial(pack_kernel, sizes[0] * at),
            [shape((sizes[at] + FLAG_ROWS * at, width + count), BF16)],
            [VMEM, VMEM, SMEM, SMEM],
            1000,
            features, probes, near_list, near_count,
        )
    far_even = moved(packed[0], -2, ((0, 0),))
    far_odd = moved(packed[0], -2, ((0, 1),))
    far_last = moved(packed[1], -2)
    own = [message]
    for level in range(1, depth + 1):
        last = level == depth
        outs = [shape((count if last else 2 * count, rank), BF16), shape((count, rank), F32)]
        message, *own = call(
            functools.partial(up_kernel, level, None if last else factors[level]),
            outs[:1] if last else outs,
            [VMEM] * 3,
            6 * rank * rank * count,
            *own, gots[-1], transfers,
        )
        gots.append(partner(message, level, SHARED[min(level, 3)]))

    tile_flops = 2 * rows * rows * (width + 4 * count)
    (near,) = call(
        functools.partial(self_kernel, scale),
        [shape((rows, count), F32)],
        [VMEM, VMEM],
        tile_flops,
        features, probes,
    )
    near, sib, xt, xst = call(
        functools.partial(pair_kernel, scale),
        [shape((rows, count), F32)] * 2 + [shape((count, rows), BF16)] * 2,
        [VMEM] * 5 + [SMEM] * 2,
        tile_flops,
        features, sib_features, near, probes, gots[0], near_list, near_count,
    )
    heads = []
    for at, (size, parts) in enumerate(zip(sizes, ((far_even, far_odd), (far_last, far_last)))):
        back_shapes = [shape((size, count), F32)] * 2 if at == 0 else [shape((rows, count), BF16)]
        near, sib, *heads = call(
            functools.partial(chunk_kernel, scale, size),
            [shape((rows, count), F32), shape((rows, count), F32), *back_shapes],
            [VMEM] * 8 + [SMEM] * 2 + [VMEM] * len(heads),
            tile_flops * 2 * size // rows,
            features, sib_features, *parts, near, sib, xt, xst, near_list, near_count, *heads,
        )
    back = moved(heads[0], 2)
    product_flops = 6 * count * rank * rank
    e3, e3_message = call(
        functools.partial(top_kernel, scale_g, factors[depth - 1]),
        [shape((count, rank), F32), shape((count, rank), BF16)],
        [VMEM] * 4,
        3 * product_flops,
        couplings, transfers, gots[depth - 1], gots[depth],
    )
    e3_sent = partner(e3_message, 2, SHARED[3])
    e2, e2_message = call(
        functools.partial(middle_kernel, scale_g, factors[2], 2),
        [shape((count, rank), F32), shape((count, rank), BF16)],
        [VMEM] * 5,
        2 * product_flops,
        couplings, transfers, gots[2], e3, e3_sent,
    )
    e2_sent = partner(e2_message, 1, SHARED[2])
    e1, sib_message = call(
        functools.partial(node_kernel, scale_g, factors[1], 1),
        [shape((count, rank), F32), shape((rows + rank, count), F32)],
        [VMEM] * 6,
        2 * product_flops,
        couplings, transfers, gots[1], e2, e2_sent, sib,
    )
    sib_got = partner(sib_message, 0)
    (far_sum,) = call(
        functools.partial(down_kernel, scale_g, factors[0]),
        [shape((rows, count), F32)],
        [VMEM] * 6,
        2 * product_flops + 6 * rows * rank * count,
        couplings, transfers, bases, gots[0], e1, sib_got,
    )
    (out,) = call(
        final_kernel,
        [shape((rows, count), F32)],
        [VMEM] * 4 + [SMEM] * 2,
        6 * rows * count,
        near, far_sum, sib_got, back, near_list, near_count,
    )
    return out


def solution(mesh):
    in_specs = (
        P("leaf", None),
        P("leaf", None),
        P("leaf", None),
        P("leaf", None, None, None),
        P("leaf", None, None, None),
        P("leaf", None),
        P("leaf"),
    )
    out_specs = P("leaf", None)
    return jax.shard_map(body, mesh=mesh, in_specs=in_specs, out_specs=out_specs, check_vma=False)
```

```python
import functools

import jax
import jax.numpy as jnp
from jax import lax
from jax.experimental import pallas as pl
from jax.experimental.pallas import tpu as pltpu
from jax.sharding import PartitionSpec as P

BF16 = jnp.bfloat16
F32 = jnp.float32
VMEM = pl.BlockSpec(memory_space=pltpu.VMEM)
SMEM = pl.BlockSpec(memory_space=pltpu.SMEM)
HBM = pl.BlockSpec(memory_space=pltpu.HBM)
ANY = pl.BlockSpec(memory_space=pl.ANY)
NN = (((1,), (0,)), ((), ()))
NT = (((1,), (1,)), ((), ()))
TN = (((0,), (0,)), ((), ()))
FLAG_ROWS = 8
LIMIT = 16 << 20
LOAD_LIMIT = 55400000
SHARED = ((), ((0, 1),), ((0, 1), (1, 0)), ((0, 1), (1, 0), (2, 1)))


def dot(a, b, dims):
    return lax.dot_general(a, b, dims, preferred_element_type=F32)


def halves(a):
    high = a.astype(BF16)
    return high, (a - high.astype(F32)).astype(BF16)


def dot_wide(a, b, dims):
    a_high, a_low = halves(a)
    b_high, b_low = halves(b)
    return dot(a_high, b_high, dims) + (dot(a_high, b_low, dims) + dot(a_low, b_high, dims))


def dot_half(a16, b, dims):
    b_high, b_low = halves(b)
    return dot(a16, b_high, dims) + dot(a16, b_low, dims)


def member(list_ref, count_ref, offset):
    index = lax.axis_index("leaf")
    found = jnp.float32(0.0)
    for slot in range(list_ref.shape[1]):
        hit = (list_ref[0, slot] == index + offset) & (slot < count_ref[0, 0])
        found = jnp.where(hit, jnp.float32(1.0), found)
    return found


def call(kernel, outs, specs, flops, *args, scratch=(), limit=LIMIT):
    out_bytes = sum(o.size * o.dtype.itemsize for o in outs)
    in_bytes = sum(a.size * a.dtype.itemsize for a in args)
    return pl.pallas_call(
        kernel,
        out_shape=outs,
        in_specs=specs,
        out_specs=[VMEM] * len(outs),
        scratch_shapes=list(scratch),
        compiler_params=pltpu.CompilerParams(vmem_limit_bytes=limit),
        cost_estimate=pl.CostEstimate(flops=flops, bytes_accessed=in_bytes + out_bytes, transcendentals=0),
    )(*args)


def load_kernel(bases_hbm, transfers_hbm, bases_ref, transfer_ref, sems):
    copies = [
        pltpu.make_async_copy(bases_hbm, bases_ref, sems.at[0]),
        pltpu.make_async_copy(transfers_hbm.at[0, 0], transfer_ref, sems.at[1]),
    ]
    for copy in copies:
        copy.start()
    for copy in copies:
        copy.wait()


def leaf_kernel(c1, bases_ref, x_ref, transfer_ref, message_ref):
    x = x_ref[...]
    rows, probes = x.shape
    skeleton = dot_wide(x, bases_ref[...], TN)
    message_ref[:probes] = skeleton
    message_ref[probes : 2 * probes] = c1 * dot_wide(skeleton, transfer_ref[...], NN)
    message_ref[2 * probes :, :probes] = x[: rows // 2]
    message_ref[2 * probes :, probes:] = x[rows // 2 :]


def pack_kernel(first, f_ref, x_ref, *refs):
    far_ref = refs[-1]
    rows, width = f_ref.shape
    probes = x_ref.shape[1]
    size = min(far_ref.shape[0], rows - first)
    far_ref[:size, :width] = f_ref[first : first + size]
    far_ref[:size, width:] = x_ref[first : first + size].astype(BF16)
    if far_ref.shape[0] > size:
        list_ref, count_ref = refs[:2]
        flags = [jnp.full((FLAG_ROWS, probes), member(list_ref, count_ref, offset), F32) for offset in (-2, -1)]
        flags.append(jnp.zeros((FLAG_ROWS, width - probes), F32))
        far_ref[size:] = jnp.concatenate(flags, axis=1).astype(BF16)


def up_kernel(level, factor, own_ref, got_ref, transfer_ref, message_ref, *next_refs):
    probes = message_ref.shape[0] if factor is None else message_ref.shape[0] // 2
    own = own_ref[probes : 2 * probes] if own_ref.shape[0] > probes else own_ref[...]
    skeleton = own + got_ref[probes : 2 * probes].astype(F32)
    message_ref[:probes] = skeleton.astype(message_ref.dtype)
    if factor is not None:
        moved = factor * dot_wide(skeleton, transfer_ref[0, level], NN)
        message_ref[probes:] = moved.astype(message_ref.dtype)
        next_refs[0][...] = moved


def bit_of(level):
    return lax.rem(lax.axis_index("leaf") >> level, 2)


def descend(scale_g, factor, got, coupling, transfer, above):
    wide = dot_wide if got.dtype == F32 else dot_half
    update = scale_g * wide(got, coupling, NT)
    return update if above is None else update + factor * dot_wide(above, transfer, NT)


def top_kernel(scale_g, factor, coupling_ref, transfer_ref, got_ref, root_ref, own_ref, message_ref):
    depth = transfer_ref.shape[1]
    probes = own_ref.shape[0]
    root = descend(scale_g, None, root_ref[...], coupling_ref[0, depth], None, None)
    out = descend(scale_g, factor, got_ref[:probes], coupling_ref[0, depth - 1], transfer_ref[0, depth - 1], root)
    own_ref[...] = out
    message_ref[...] = out.astype(BF16)


def middle_kernel(scale_g, factor, level, coupling_ref, transfer_ref, got_ref, above_ref, sent_ref, own_ref, message_ref):
    probes = own_ref.shape[0]
    above = jnp.where(bit_of(level) == 1, above_ref[...], sent_ref[...].astype(F32))
    out = descend(scale_g, factor, got_ref[:probes], coupling_ref[0, level], transfer_ref[0, level], above)
    own_ref[...] = out
    message_ref[...] = out.astype(BF16)


def node_kernel(scale_g, factor, level, coupling_ref, transfer_ref, got_ref, above_ref, sent_ref, cross_ref, pair_ref, own_ref, message_ref):
    probes, rank = own_ref.shape
    at = 2 * cross_ref.shape[0]
    message_ref[: at // 2] = cross_ref[...]
    message_ref[at // 2 : at] = pair_ref[...]
    above = jnp.where(bit_of(level) == 0, above_ref[...], sent_ref[...].astype(F32))
    out = descend(scale_g, factor, got_ref[:probes], coupling_ref[0, level], transfer_ref[0, level], above)
    own_ref[...] = out
    for part in halves(out):
        for first in range(0, rank, probes):
            message_ref[at : at + probes] = part[:, first : first + probes]
            at += probes


def down_kernel(scale_g, factor, coupling_ref, transfer_ref, bases_ref, got_ref, above_ref, sent_ref, out_ref):
    rows, probes = out_ref.shape
    rank = bases_ref.shape[1]
    high, low = [
        jnp.concatenate([sent_ref[at + first : at + first + probes] for first in range(0, rank, probes)], axis=1).astype(F32)
        for at in (2 * rows, 2 * rows + rank)
    ]
    above = jnp.where(bit_of(0) == 1, above_ref[...], high + low)
    expansion = descend(scale_g, factor, got_ref[:probes], coupling_ref[0, 0], transfer_ref[0, 0], above)
    out_ref[...] = dot_wide(bases_ref[...], expansion, NT)


def tile(rows_a, rows_b, scale):
    gram = dot(rows_a, rows_b, NT)
    return halves(gram * gram * scale)


def self_kernel(scale, f_ref, x_ref, out_ref):
    high, low = tile(f_ref[...], f_ref[...], scale)
    x_high, x_low = halves(x_ref[...])
    out_ref[...] = dot(high, x_high, NN) + (dot(high, x_low, NN) + dot(low, x_high, NN))


def times(parts, x16):
    return dot(parts[0], x16, NN) + dot(parts[1], x16, NN)


def times_back(parts, xt16):
    return (dot(xt16, parts[0], NN) + dot(xt16, parts[1], NN)).T


def pair_kernel(scale, f_ref, g_ref, near_ref, x_ref, got_ref, list_ref, count_ref, out_ref, pair_ref, xt_ref, xst_ref):
    even = bit_of(0) == 0
    rows, probes = near_ref.shape
    xt_ref[...] = x_ref[...].T.astype(BF16)
    halves_of = [got_ref[2 * probes :, half * probes : (half + 1) * probes] for half in range(2)]
    for half, part in enumerate(halves_of):
        xst_ref[:, half * (rows // 2) : (half + 1) * (rows // 2)] = part.T.astype(BF16)

    @pl.when(even)
    def _():
        parts = tile(f_ref[...], g_ref[...], scale)
        flag = member(list_ref, count_ref, 1)
        out_ref[...] = near_ref[...] + flag * times(parts, jnp.concatenate(halves_of, axis=0).astype(BF16))
        pair_ref[...] = times_back(parts, xt_ref[...]).astype(BF16)

    @pl.when(jnp.logical_not(even))
    def _():
        out_ref[...] = near_ref[...]
        pair_ref[...] = jnp.zeros_like(pair_ref)


def chunk_kernel(scale, size, f_ref, g_ref, far_ref, near_ref, xt_ref, xst_ref, list_ref, count_ref, *refs):
    even = lax.rem(lax.axis_index("leaf"), 2) == 0
    width = f_ref.shape[1]
    probes = near_ref.shape[1]
    heads = refs[: len(refs) // 5 * 3]
    out_ref, sib_ref, *back_refs = refs[len(heads) :]
    mine = member(list_ref, count_ref, 2)

    def put(back, cross_back):
        if not heads:
            back_refs[0][...] = back
            back_refs[1][...] = jnp.zeros_like(back) if cross_back is None else cross_back
            return
        head = heads[1].shape[0]
        flag2 = far_ref[size : size + 1, :probes].astype(F32)
        flag1 = far_ref[size : size + 1, probes : 2 * probes].astype(F32)
        back_refs[0][:head] = (flag2 * heads[1][...] + flag1 * heads[2][...]).astype(BF16)
        total = flag2 * back
        back_refs[0][head:] = (total if cross_back is None else total + flag1 * cross_back).astype(BF16)

    @pl.when(even)
    def _():
        h = far_ref[:size, :width]
        xh = far_ref[:size, width:]
        parts = tile(f_ref[...], h, scale)
        out_ref[...] = near_ref[...] + mine * times(parts, xh)
        cross = tile(g_ref[...], h, scale)
        sib = times(cross, xh)
        sib_ref[...] = (sib + heads[0][...] if heads else sib).astype(sib_ref.dtype)
        put(times_back(parts, xt_ref[...]), times_back(cross, xst_ref[...]))

    @pl.when(jnp.logical_not(even))
    def _():
        h = far_ref[:size, :width]
        xh = far_ref[:size, width:]
        parts = tile(f_ref[...], h, scale)
        out_ref[...] = near_ref[...] + mine * times(parts, xh)
        sib_ref[...] = jnp.zeros_like(sib_ref)
        put(times_back(parts, xt_ref[...]), None)


def final_kernel(near_ref, far_ref, sib_ref, back_ref, list_ref, count_ref, out_ref):
    rows = out_ref.shape[0]
    after, before = member(list_ref, count_ref, 1), member(list_ref, count_ref, -1)
    sib = after * sib_ref[:rows].astype(F32) + before * sib_ref[rows : 2 * rows].astype(F32)
    out_ref[...] = near_ref[...] + far_ref[...] + sib + back_ref[...].astype(F32)


def sender(index, bits):
    return all(index >> at & 1 == bit for at, bit in bits)


def moved(array, by, wrap=True):
    peers = lax.axis_size("leaf")
    return lax.ppermute(array, "leaf", [(i, (i + by) % peers) for i in range(peers) if wrap or 0 <= i + by < peers])


def level1_partner(index):
    return index ^ (2 if index & 1 else 8 if index & 2 else 4)


def across(array, distance, bits=()):
    senders = [i for i in range(lax.axis_size("leaf")) if sender(i, bits)]
    return lax.ppermute(array, "leaf", [(i, i ^ distance) for i in senders])


def partner(array, level, bits=()):
    return across(array, 1 << level, bits)


def body(features, probes, bases, transfers, couplings, near_list, near_count):
    rows, width = features.shape
    near_count = near_count.reshape(1, 1)
    count = probes.shape[1]
    rank = bases.shape[1]
    depth = transfers.shape[1]
    scale = 1.0 / (rows * width)
    scale_g = (3.0 / rank) ** 0.5
    factors = [scale_g * 2.0 ** (-0.5 * (level + 1)) for level in range(depth)]
    shape = jax.ShapeDtypeStruct
    sizes = [rows // 2, rows // 2]

    sib_features = partner(features, 0)
    bases_v, transfer0 = call(
        load_kernel,
        [shape((rows, rank), F32), shape((rank, rank), F32)],
        [HBM] * 2,
        1000,
        bases, transfers,
        scratch=[pltpu.SemaphoreType.DMA((2,))],
        limit=LOAD_LIMIT,
    )
    (message,) = call(
        functools.partial(leaf_kernel, factors[0]),
        [shape((2 * count + rows // 2, rank), F32)],
        [VMEM] * 3,
        6 * rows * rank * count,
        bases_v, probes, transfer0,
    )
    gots = [partner(message, 0)]
    packed = []
    for at, lists in enumerate(([], [near_list, near_count])):
        packed += call(
            functools.partial(pack_kernel, sizes[0] * at),
            [shape((sizes[at] + FLAG_ROWS * at, width + count), BF16)],
            [VMEM, VMEM] + [SMEM] * len(lists),
            1000,
            features, probes, *lists,
        )
    far_first = moved(packed[0], -2)
    far_last = moved(packed[1], -2, wrap=False)
    own = [message]
    for level in range(1, depth + 1):
        last = level == depth
        outs = [shape((count if last else 2 * count, rank), BF16), shape((count, rank), F32)]
        message, *own = call(
            functools.partial(up_kernel, level, None if last else factors[level]),
            outs[:1] if last else outs,
            [VMEM] * 3,
            6 * rank * rank * count,
            *own, gots[-1], transfers,
        )
        if level == 1:
            whole = [(i, level1_partner(i)) for i in range(lax.axis_size("leaf"))]
            gots.append(lax.ppermute(message, "leaf", whole))
        else:
            gots.append(partner(message, level, SHARED[min(level, 3)]))

    tile_flops = 2 * rows * rows * (width + 4 * count)
    (near,) = call(
        functools.partial(self_kernel, scale),
        [shape((rows, count), F32)],
        [VMEM, VMEM],
        tile_flops,
        features, probes,
    )
    near, pair, xt, xst = call(
        functools.partial(pair_kernel, scale),
        [shape((rows, count), F32), shape((rows, count), BF16)] + [shape((count, rows), BF16)] * 2,
        [VMEM] * 5 + [SMEM] * 2,
        tile_flops,
        features, sib_features, near, probes, gots[0], near_list, near_count,
    )
    heads = []
    for at, (size, part) in enumerate(zip(sizes, (far_first, far_last))):
        back_shapes = [shape((size, count), F32)] * 2 if at == 0 else [shape((rows, count), BF16)]
        near, *heads = call(
            functools.partial(chunk_kernel, scale, size),
            [shape((rows, count), F32), shape((rows, count), BF16 if at else F32), *back_shapes],
            [VMEM] * 6 + [SMEM] * 2 + [VMEM] * len(heads),
            tile_flops * 2 * size // rows,
            features, sib_features, part, near, xt, xst, near_list, near_count, *heads,
        )
    cross, back = heads
    back = moved(back, 2, wrap=False)
    product_flops = 6 * count * rank * rank
    e3, e3_message = call(
        functools.partial(top_kernel, scale_g, factors[depth - 1]),
        [shape((count, rank), F32), shape((count, rank), BF16)],
        [VMEM] * 4,
        3 * product_flops,
        couplings, transfers, gots[depth - 1], gots[depth],
    )
    e3_sent = partner(e3_message, 2, SHARED[3])
    e2, e2_message = call(
        functools.partial(middle_kernel, scale_g, factors[2], 2),
        [shape((count, rank), F32), shape((count, rank), BF16)],
        [VMEM] * 5,
        2 * product_flops,
        couplings, transfers, gots[2], e3, e3_sent,
    )
    e2_sent = partner(e2_message, 1, SHARED[2])
    e1, sib_message = call(
        functools.partial(node_kernel, scale_g, factors[1], 1),
        [shape((count, rank), F32), shape((2 * rows + 2 * rank, count), BF16)],
        [VMEM] * 7,
        2 * product_flops,
        couplings, transfers, gots[1], e2, e2_sent, cross, pair,
    )
    sib_got = partner(sib_message, 0)
    (far_sum,) = call(
        functools.partial(down_kernel, scale_g, factors[0]),
        [shape((rows, count), F32)],
        [VMEM] * 6,
        2 * product_flops + 6 * rows * rank * count,
        couplings, transfers, bases_v, gots[0], e1, sib_got,
    )
    (out,) = call(
        final_kernel,
        [shape((rows, count), F32)],
        [VMEM] * 4 + [SMEM] * 2,
        6 * rows * count,
        near, far_sum, sib_got, back, near_list, near_count,
    )
    return out


def solution(mesh):
    in_specs = (
        P("leaf", None),
        P("leaf", None),
        P("leaf", None),
        P("leaf", None, None, None),
        P("leaf", None, None, None),
        P("leaf", None),
        P("leaf"),
    )
    out_specs = P("leaf", None)
    return jax.shard_map(body, mesh=mesh, in_specs=in_specs, out_specs=out_specs, check_vma=False)
```

```python
import functools

import jax
import jax.numpy as jnp
from jax import lax
from jax.experimental import pallas as pl
from jax.experimental.pallas import tpu as pltpu
from jax.sharding import PartitionSpec as P

BF16 = jnp.bfloat16
F32 = jnp.float32
VMEM = pl.BlockSpec(memory_space=pltpu.VMEM)
SMEM = pl.BlockSpec(memory_space=pltpu.SMEM)
HBM = pl.BlockSpec(memory_space=pltpu.HBM)
ANY = pl.BlockSpec(memory_space=pl.ANY)
NN = (((1,), (0,)), ((), ()))
NT = (((1,), (1,)), ((), ()))
TN = (((0,), (0,)), ((), ()))
FLAG_ROWS = 8
OFFSETS = (-2, -1, 1, 2)
LIMIT = 16 << 20
LOAD_LIMIT = 55400000
SHARED = ((), ((0, 1),), ((0, 1), (1, 0)), ((0, 1), (1, 0), (2, 1)))


def dot(a, b, dims):
    return lax.dot_general(a, b, dims, preferred_element_type=F32)


def halves(a):
    high = a.astype(BF16)
    return high, (a - high.astype(F32)).astype(BF16)


def dot_wide(a, b, dims):
    a_high, a_low = halves(a)
    b_high, b_low = halves(b)
    return dot(a_high, b_high, dims) + (dot(a_high, b_low, dims) + dot(a_low, b_high, dims))


def dot_half(a16, b, dims):
    b_high, b_low = halves(b)
    return dot(a16, b_high, dims) + dot(a16, b_low, dims)


def member(list_ref, count_ref, offset):
    index = lax.axis_index("leaf")
    found = jnp.float32(0.0)
    for slot in range(list_ref.shape[1]):
        hit = (list_ref[0, slot] == index + offset) & (slot < count_ref[0, 0])
        found = jnp.where(hit, jnp.float32(1.0), found)
    return found


def call(kernel, outs, specs, flops, *args, scratch=(), limit=LIMIT):
    out_bytes = sum(o.size * o.dtype.itemsize for o in outs)
    in_bytes = sum(a.size * a.dtype.itemsize for a in args)
    return pl.pallas_call(
        kernel,
        out_shape=outs,
        in_specs=specs,
        out_specs=[VMEM] * len(outs),
        scratch_shapes=list(scratch),
        compiler_params=pltpu.CompilerParams(vmem_limit_bytes=limit),
        cost_estimate=pl.CostEstimate(flops=flops, bytes_accessed=in_bytes + out_bytes, transcendentals=0),
    )(*args)


def load_kernel(bases_hbm, transfers_hbm, bases_ref, transfer_ref, sems):
    copies = [
        pltpu.make_async_copy(bases_hbm, bases_ref, sems.at[0]),
        pltpu.make_async_copy(transfers_hbm.at[0, 0], transfer_ref, sems.at[1]),
    ]
    for copy in copies:
        copy.start()
    for copy in copies:
        copy.wait()


def leaf_kernel(c1, bases_ref, x_ref, transfer_ref, message_ref):
    x = x_ref[...]
    rows, probes = x.shape
    skeleton = dot_wide(x, bases_ref[...], TN)
    message_ref[:probes] = skeleton
    message_ref[probes : 2 * probes] = c1 * dot_wide(skeleton, transfer_ref[...], NN)
    message_ref[2 * probes :, :probes] = x[: rows // 2]
    message_ref[2 * probes :, probes:] = x[rows // 2 :]


def pack_kernel(first, f_ref, x_ref, *refs):
    rows, width = f_ref.shape
    probes = x_ref.shape[1]
    if len(refs) == 1:
        far_ref = refs[0]
        size = far_ref.shape[0]
    else:
        list_ref, count_ref, far_ref, flags_ref = refs
        size = rows - first
        flags = [jnp.full((FLAG_ROWS, probes), member(list_ref, count_ref, offset), F32) for offset in (-2, -1)]
        flags.append(jnp.zeros((FLAG_ROWS, width - probes), F32))
        far_ref[size:] = jnp.concatenate(flags, axis=1).astype(BF16)
        for row, offset in enumerate(OFFSETS):
            flags_ref[row : row + 1] = jnp.full((1, probes), member(list_ref, count_ref, offset), F32)
    far_ref[:size, :width] = f_ref[first : first + size]
    far_ref[:size, width:] = x_ref[first : first + size].astype(BF16)


def flag_of(flags_ref, offset):
    row = OFFSETS.index(offset)
    return flags_ref[row : row + 1]


def up_kernel(level, factor, own_ref, got_ref, transfer_ref, message_ref, *next_refs):
    probes = message_ref.shape[0] if factor is None else message_ref.shape[0] // 2
    own = own_ref[probes : 2 * probes] if own_ref.shape[0] > probes else own_ref[...]
    skeleton = own + got_ref[probes : 2 * probes].astype(F32)
    message_ref[:probes] = skeleton.astype(message_ref.dtype)
    if factor is not None:
        moved = factor * dot_wide(skeleton, transfer_ref[0, level], NN)
        message_ref[probes:] = moved.astype(message_ref.dtype)
        next_refs[0][...] = moved


def bit_of(level):
    return lax.rem(lax.axis_index("leaf") >> level, 2)


def descend(scale_g, factor, got, coupling, transfer, above):
    wide = dot_wide if got.dtype == F32 else dot_half
    update = scale_g * wide(got, coupling, NT)
    return update if above is None else update + factor * dot_wide(above, transfer, NT)


def top_kernel(scale_g, factor, coupling_ref, transfer_ref, got_ref, root_ref, own_ref, message_ref):
    depth = transfer_ref.shape[1]
    probes = own_ref.shape[0]
    root = descend(scale_g, None, root_ref[...], coupling_ref[0, depth], None, None)
    out = descend(scale_g, factor, got_ref[:probes], coupling_ref[0, depth - 1], transfer_ref[0, depth - 1], root)
    own_ref[...] = out
    message_ref[...] = out.astype(BF16)


def middle_kernel(scale_g, factor, level, coupling_ref, transfer_ref, got_ref, above_ref, sent_ref, own_ref, message_ref):
    probes = own_ref.shape[0]
    above = jnp.where(bit_of(level) == 1, above_ref[...], sent_ref[...].astype(F32))
    out = descend(scale_g, factor, got_ref[:probes], coupling_ref[0, level], transfer_ref[0, level], above)
    own_ref[...] = out
    message_ref[...] = out.astype(BF16)


def node_kernel(scale_g, factor, level, coupling_ref, transfer_ref, got_ref, above_ref, sent_ref, cross_ref, pair_ref, own_ref, message_ref):
    probes, rank = own_ref.shape
    at = 2 * cross_ref.shape[0]
    message_ref[: at // 2] = cross_ref[...]
    message_ref[at // 2 : at] = pair_ref[...]
    above = jnp.where(bit_of(level) == 0, above_ref[...], sent_ref[...].astype(F32))
    out = descend(scale_g, factor, got_ref[:probes], coupling_ref[0, level], transfer_ref[0, level], above)
    own_ref[...] = out
    for part in halves(out):
        for first in range(0, rank, probes):
            message_ref[at : at + probes] = part[:, first : first + probes]
            at += probes


def down_kernel(scale_g, factor, coupling_ref, transfer_ref, bases_ref, got_ref, above_ref, sent_ref, out_ref):
    rows, probes = out_ref.shape
    rank = bases_ref.shape[1]
    high, low = [
        jnp.concatenate([sent_ref[at + first : at + first + probes] for first in range(0, rank, probes)], axis=1).astype(F32)
        for at in (2 * rows, 2 * rows + rank)
    ]
    above = jnp.where(bit_of(0) == 1, above_ref[...], high + low)
    expansion = descend(scale_g, factor, got_ref[:probes], coupling_ref[0, 0], transfer_ref[0, 0], above)
    out_ref[...] = dot_wide(bases_ref[...], expansion, NT)


def tile(rows_a, rows_b, scale):
    gram = dot(rows_a, rows_b, NT)
    return halves(gram * gram * scale)


def self_kernel(scale, f_ref, x_ref, out_ref):
    high, low = tile(f_ref[...], f_ref[...], scale)
    x_high, x_low = halves(x_ref[...])
    out_ref[...] = dot(high, x_high, NN) + (dot(high, x_low, NN) + dot(low, x_high, NN))


def times(parts, x16):
    return dot(parts[0], x16, NN) + dot(parts[1], x16, NN)


def times_back(parts, xt16):
    return (dot(xt16, parts[0], NN) + dot(xt16, parts[1], NN)).T


def pair_kernel(scale, f_ref, g_ref, near_ref, x_ref, got_ref, flags_ref, out_ref, pair_ref, xt_ref, xst_ref):
    even = bit_of(0) == 0
    rows, probes = near_ref.shape
    xt_ref[...] = x_ref[...].T.astype(BF16)
    halves_of = [got_ref[2 * probes :, half * probes : (half + 1) * probes] for half in range(2)]
    for half, part in enumerate(halves_of):
        xst_ref[:, half * (rows // 2) : (half + 1) * (rows // 2)] = part.T.astype(BF16)

    @pl.when(even)
    def _():
        parts = tile(f_ref[...], g_ref[...], scale)
        flag = flag_of(flags_ref, 1)
        out_ref[...] = near_ref[...] + flag * times(parts, jnp.concatenate(halves_of, axis=0).astype(BF16))
        pair_ref[...] = times_back(parts, xt_ref[...]).astype(BF16)

    @pl.when(jnp.logical_not(even))
    def _():
        out_ref[...] = near_ref[...]
        pair_ref[...] = jnp.zeros_like(pair_ref)


def chunk_kernel(scale, size, f_ref, g_ref, far_ref, near_ref, xt_ref, xst_ref, flags_ref, *refs):
    even = lax.rem(lax.axis_index("leaf"), 2) == 0
    width = f_ref.shape[1]
    probes = near_ref.shape[1]
    heads = refs[: len(refs) // 5 * 3]
    out_ref, sib_ref, *back_refs = refs[len(heads) :]
    mine = flag_of(flags_ref, 2)

    def put(back, cross_back):
        if not heads:
            back_refs[0][...] = back
            back_refs[1][...] = jnp.zeros_like(back) if cross_back is None else cross_back
            return
        head = heads[1].shape[0]
        flag2 = far_ref[size : size + 1, :probes].astype(F32)
        flag1 = far_ref[size : size + 1, probes : 2 * probes].astype(F32)
        back_refs[0][:head] = (flag2 * heads[1][...] + flag1 * heads[2][...]).astype(BF16)
        total = flag2 * back
        back_refs[0][head:] = (total if cross_back is None else total + flag1 * cross_back).astype(BF16)

    @pl.when(even)
    def _():
        h = far_ref[:size, :width]
        xh = far_ref[:size, width:]
        parts = tile(f_ref[...], h, scale)
        out_ref[...] = near_ref[...] + mine * times(parts, xh)
        cross = tile(g_ref[...], h, scale)
        sib = times(cross, xh)
        sib_ref[...] = (sib + heads[0][...] if heads else sib).astype(sib_ref.dtype)
        put(times_back(parts, xt_ref[...]), times_back(cross, xst_ref[...]))

    @pl.when(jnp.logical_not(even))
    def _():
        h = far_ref[:size, :width]
        xh = far_ref[:size, width:]
        parts = tile(f_ref[...], h, scale)
        out_ref[...] = near_ref[...] + mine * times(parts, xh)
        sib_ref[...] = jnp.zeros_like(sib_ref)
        put(times_back(parts, xt_ref[...]), None)


def final_kernel(near_ref, far_ref, sib_ref, back_ref, flags_ref, out_ref):
    rows = out_ref.shape[0]
    after, before = flag_of(flags_ref, 1), flag_of(flags_ref, -1)
    sib = after * sib_ref[:rows].astype(F32) + before * sib_ref[rows : 2 * rows].astype(F32)
    out_ref[...] = near_ref[...] + far_ref[...] + sib + back_ref[...].astype(F32)


def sender(index, bits):
    return all(index >> at & 1 == bit for at, bit in bits)


def moved(array, by, wrap=True):
    peers = lax.axis_size("leaf")
    return lax.ppermute(array, "leaf", [(i, (i + by) % peers) for i in range(peers) if wrap or 0 <= i + by < peers])


def level1_partner(index):
    return index ^ (2 if index & 1 else 8 if index & 2 else 4)


def across(array, distance, bits=()):
    senders = [i for i in range(lax.axis_size("leaf")) if sender(i, bits)]
    return lax.ppermute(array, "leaf", [(i, i ^ distance) for i in senders])


def partner(array, level, bits=()):
    return across(array, 1 << level, bits)


def body(features, probes, bases, transfers, couplings, near_list, near_count):
    rows, width = features.shape
    near_count = near_count.reshape(1, 1)
    count = probes.shape[1]
    rank = bases.shape[1]
    depth = transfers.shape[1]
    scale = 1.0 / (rows * width)
    scale_g = (3.0 / rank) ** 0.5
    factors = [scale_g * 2.0 ** (-0.5 * (level + 1)) for level in range(depth)]
    shape = jax.ShapeDtypeStruct
    sizes = [rows // 2, rows // 2]

    sib_features = partner(features, 0)
    bases_v, transfer0 = call(
        load_kernel,
        [shape((rows, rank), F32), shape((rank, rank), F32)],
        [HBM] * 2,
        1000,
        bases, transfers,
        scratch=[pltpu.SemaphoreType.DMA((2,))],
        limit=LOAD_LIMIT,
    )
    (message,) = call(
        functools.partial(leaf_kernel, factors[0]),
        [shape((2 * count + rows // 2, rank), F32)],
        [VMEM] * 3,
        6 * rows * rank * count,
        bases_v, probes, transfer0,
    )
    gots = [partner(message, 0)]
    packed = []
    for at, lists in enumerate(([], [near_list, near_count])):
        packed += call(
            functools.partial(pack_kernel, sizes[0] * at),
            [shape((sizes[at] + FLAG_ROWS * at, width + count), BF16)] + [shape((FLAG_ROWS, count), F32)] * at,
            [VMEM, VMEM] + [SMEM] * len(lists),
            1000,
            features, probes, *lists,
        )
    flags = packed.pop()
    far_first = moved(packed[0], -2)
    far_last = moved(packed[1], -2, wrap=False)
    own = [message]
    for level in range(1, depth + 1):
        last = level == depth
        outs = [shape((count if last else 2 * count, rank), BF16), shape((count, rank), F32)]
        message, *own = call(
            functools.partial(up_kernel, level, None if last else factors[level]),
            outs[:1] if last else outs,
            [VMEM] * 3,
            6 * rank * rank * count,
            *own, gots[-1], transfers,
        )
        if level == 1:
            whole = [(i, level1_partner(i)) for i in range(lax.axis_size("leaf"))]
            gots.append(lax.ppermute(message, "leaf", whole))
        else:
            gots.append(partner(message, level, SHARED[min(level, 3)]))

    tile_flops = 2 * rows * rows * (width + 4 * count)
    (near,) = call(
        functools.partial(self_kernel, scale),
        [shape((rows, count), F32)],
        [VMEM, VMEM],
        tile_flops,
        features, probes,
    )
    near, pair, xt, xst = call(
        functools.partial(pair_kernel, scale),
        [shape((rows, count), F32), shape((rows, count), BF16)] + [shape((count, rows), BF16)] * 2,
        [VMEM] * 6,
        tile_flops,
        features, sib_features, near, probes, gots[0], flags,
    )
    heads = []
    for at, (size, part) in enumerate(zip(sizes, (far_first, far_last))):
        back_shapes = [shape((size, count), F32)] * 2 if at == 0 else [shape((rows, count), BF16)]
        near, *heads = call(
            functools.partial(chunk_kernel, scale, size),
            [shape((rows, count), F32), shape((rows, count), BF16 if at else F32), *back_shapes],
            [VMEM] * (7 + len(heads)),
            tile_flops * 2 * size // rows,
            features, sib_features, part, near, xt, xst, flags, *heads,
        )
    cross, back = heads
    back = moved(back, 2, wrap=False)
    product_flops = 6 * count * rank * rank
    e3, e3_message = call(
        functools.partial(top_kernel, scale_g, factors[depth - 1]),
        [shape((count, rank), F32), shape((count, rank), BF16)],
        [VMEM] * 4,
        3 * product_flops,
        couplings, transfers, gots[depth - 1], gots[depth],
    )
    e3_sent = partner(e3_message, 2, SHARED[3])
    e2, e2_message = call(
        functools.partial(middle_kernel, scale_g, factors[2], 2),
        [shape((count, rank), F32), shape((count, rank), BF16)],
        [VMEM] * 5,
        2 * product_flops,
        couplings, transfers, gots[2], e3, e3_sent,
    )
    e2_sent = partner(e2_message, 1, SHARED[2])
    e1, sib_message = call(
        functools.partial(node_kernel, scale_g, factors[1], 1),
        [shape((count, rank), F32), shape((2 * rows + 2 * rank, count), BF16)],
        [VMEM] * 7,
        2 * product_flops,
        couplings, transfers, gots[1], e2, e2_sent, cross, pair,
    )
    sib_got = partner(sib_message, 0)
    (far_sum,) = call(
        functools.partial(down_kernel, scale_g, factors[0]),
        [shape((rows, count), F32)],
        [VMEM] * 6,
        2 * product_flops + 6 * rows * rank * count,
        couplings, transfers, bases_v, gots[0], e1, sib_got,
    )
    (out,) = call(
        final_kernel,
        [shape((rows, count), F32)],
        [VMEM] * 5,
        6 * rows * count,
        near, far_sum, sib_got, back, flags,
    )
    return out


def solution(mesh):
    in_specs = (
        P("leaf", None),
        P("leaf", None),
        P("leaf", None),
        P("leaf", None, None, None),
        P("leaf", None, None, None),
        P("leaf", None),
        P("leaf"),
    )
    out_specs = P("leaf", None)
    return jax.shard_map(body, mesh=mesh, in_specs=in_specs, out_specs=out_specs, check_vma=False)
```

```python
import functools

import jax
import jax.numpy as jnp
from jax import lax
from jax.experimental import pallas as pl
from jax.experimental.pallas import tpu as pltpu
from jax.sharding import PartitionSpec as P

BF16 = jnp.bfloat16
F32 = jnp.float32
VMEM = pl.BlockSpec(memory_space=pltpu.VMEM)
HBM = pl.BlockSpec(memory_space=pltpu.HBM)
ANY = pl.BlockSpec(memory_space=pl.ANY)
NN = (((1,), (0,)), ((), ()))
NT = (((1,), (1,)), ((), ()))
TN = (((0,), (0,)), ((), ()))
FLAG_ROWS = 8
OFFSETS = (-2, -1, 1, 2)
LIMIT = 16 << 20
LOAD_LIMIT = 55400000
SHARED = ((), ((0, 1),), ((0, 1), (1, 0)), ((0, 1), (1, 0), (2, 1)))


def dot(a, b, dims):
    return lax.dot_general(a, b, dims, preferred_element_type=F32)


def halves(a):
    high = a.astype(BF16)
    return high, (a - high.astype(F32)).astype(BF16)


def dot_wide(a, b, dims):
    a_high, a_low = halves(a)
    b_high, b_low = halves(b)
    return dot(a_high, b_high, dims) + (dot(a_high, b_low, dims) + dot(a_low, b_high, dims))


def dot_half(a16, b, dims):
    b_high, b_low = halves(b)
    return dot(a16, b_high, dims) + dot(a16, b_low, dims)


def member(near_list, near_count, offset):
    slots = lax.broadcasted_iota(jnp.int32, near_list.shape, 1)
    hits = (near_list == lax.axis_index("leaf") + offset) & (slots < near_count)
    return jnp.max(jnp.where(hits, jnp.float32(1.0), jnp.float32(0.0)), axis=1, keepdims=True)


def call(kernel, outs, specs, flops, *args, scratch=(), limit=LIMIT):
    out_bytes = sum(o.size * o.dtype.itemsize for o in outs)
    in_bytes = sum(a.size * a.dtype.itemsize for a in args)
    return pl.pallas_call(
        kernel,
        out_shape=outs,
        in_specs=specs,
        out_specs=[VMEM] * len(outs),
        scratch_shapes=list(scratch),
        compiler_params=pltpu.CompilerParams(vmem_limit_bytes=limit),
        cost_estimate=pl.CostEstimate(flops=flops, bytes_accessed=in_bytes + out_bytes, transcendentals=0),
    )(*args)


def load_kernel(bases_hbm, transfers_hbm, bases_ref, transfer_ref, sems):
    copies = [
        pltpu.make_async_copy(bases_hbm, bases_ref, sems.at[0]),
        pltpu.make_async_copy(transfers_hbm.at[0, 0], transfer_ref, sems.at[1]),
    ]
    for copy in copies:
        copy.start()
    for copy in copies:
        copy.wait()


def leaf_kernel(c1, bases_ref, x_ref, transfer_ref, message_ref):
    x = x_ref[...]
    probes = x.shape[1]
    skeleton = dot_wide(x, bases_ref[...], TN)
    message_ref[:probes] = skeleton
    message_ref[probes:] = c1 * dot_wide(skeleton, transfer_ref[...], NN)


def pack_kernel(first, f_ref, x_ref, *refs):
    rows, width = f_ref.shape
    probes = x_ref.shape[1]
    if len(refs) == 1:
        far_ref = refs[0]
        size = far_ref.shape[0]
    else:
        list_ref, far_ref, flags_ref, x16_ref = refs
        size = rows - first
        slots = list_ref.shape[1] - 1
        found = [member(list_ref[:, :slots], list_ref[:, slots:], offset) for offset in OFFSETS]
        flags = [jnp.broadcast_to(flag, (FLAG_ROWS, probes)) for flag in found[:2]]
        flags.append(jnp.zeros((FLAG_ROWS, width - probes), F32))
        far_ref[size:] = jnp.concatenate(flags, axis=1).astype(BF16)
        for row, flag in enumerate(found):
            flags_ref[row : row + 1] = jnp.broadcast_to(flag, (1, probes))
        x16_ref[...] = x_ref[...].astype(BF16)
    far_ref[:size, :width] = f_ref[first : first + size]
    far_ref[:size, width:] = x_ref[first : first + size].astype(BF16)


def flag_of(flags_ref, offset):
    row = OFFSETS.index(offset)
    return flags_ref[row : row + 1]


def up_kernel(level, factor, own_ref, got_ref, transfer_ref, message_ref, *next_refs):
    probes = message_ref.shape[0] if factor is None else message_ref.shape[0] // 2
    own = own_ref[probes : 2 * probes] if own_ref.shape[0] > probes else own_ref[...]
    skeleton = own + got_ref[probes : 2 * probes].astype(F32)
    message_ref[:probes] = skeleton.astype(message_ref.dtype)
    if factor is not None:
        moved = factor * dot_wide(skeleton, transfer_ref[0, level], NN)
        message_ref[probes:] = moved.astype(message_ref.dtype)
        next_refs[0][...] = moved


def bit_of(level):
    return lax.rem(lax.axis_index("leaf") >> level, 2)


def descend(scale_g, factor, got, coupling, transfer, above):
    wide = dot_wide if got.dtype == F32 else dot_half
    update = scale_g * wide(got, coupling, NT)
    return update if above is None else update + factor * dot_wide(above, transfer, NT)


def top_kernel(scale_g, factor, coupling_ref, transfer_ref, got_ref, root_ref, own_ref, message_ref):
    depth = transfer_ref.shape[1]
    probes = own_ref.shape[0]
    root = descend(scale_g, None, root_ref[...], coupling_ref[0, depth], None, None)
    out = descend(scale_g, factor, got_ref[:probes], coupling_ref[0, depth - 1], transfer_ref[0, depth - 1], root)
    own_ref[...] = out
    message_ref[...] = out.astype(BF16)


def middle_kernel(scale_g, factor, level, coupling_ref, transfer_ref, got_ref, above_ref, sent_ref, own_ref, message_ref):
    probes = own_ref.shape[0]
    above = jnp.where(bit_of(level) == 1, above_ref[...], sent_ref[...].astype(F32))
    out = descend(scale_g, factor, got_ref[:probes], coupling_ref[0, level], transfer_ref[0, level], above)
    own_ref[...] = out
    message_ref[...] = out.astype(BF16)


def node_kernel(scale_g, factor, level, coupling_ref, transfer_ref, got_ref, above_ref, sent_ref, cross_ref, pair_ref, own_ref, message_ref):
    probes, rank = own_ref.shape
    at = 2 * cross_ref.shape[0]
    message_ref[: at // 2] = cross_ref[...]
    message_ref[at // 2 : at] = pair_ref[...]
    above = jnp.where(bit_of(level) == 0, above_ref[...], sent_ref[...].astype(F32))
    out = descend(scale_g, factor, got_ref[:probes], coupling_ref[0, level], transfer_ref[0, level], above)
    own_ref[...] = out
    for part in halves(out):
        for first in range(0, rank, probes):
            message_ref[at : at + probes] = part[:, first : first + probes]
            at += probes


def down_kernel(scale_g, factor, coupling_ref, transfer_ref, bases_ref, got_ref, above_ref, sent_ref, out_ref):
    rows, probes = out_ref.shape
    rank = bases_ref.shape[1]
    high, low = [
        jnp.concatenate([sent_ref[at + first : at + first + probes] for first in range(0, rank, probes)], axis=1).astype(F32)
        for at in (2 * rows, 2 * rows + rank)
    ]
    above = jnp.where(bit_of(0) == 1, above_ref[...], high + low)
    expansion = descend(scale_g, factor, got_ref[:probes], coupling_ref[0, 0], transfer_ref[0, 0], above)
    out_ref[...] = dot_wide(bases_ref[...], expansion, NT)


def tile(rows_a, rows_b, scale):
    gram = dot(rows_a, rows_b, NT)
    return halves(gram * gram * scale)


def self_kernel(scale, f_ref, x_ref, out_ref):
    high, low = tile(f_ref[...], f_ref[...], scale)
    x_high, x_low = halves(x_ref[...])
    out_ref[...] = dot(high, x_high, NN) + (dot(high, x_low, NN) + dot(low, x_high, NN))


def times(parts, x16):
    return dot(parts[0], x16, NN) + dot(parts[1], x16, NN)


def times_back(parts, xt16):
    return (dot(xt16, parts[0], NN) + dot(xt16, parts[1], NN)).T


def pair_kernel(scale, f_ref, g_ref, near_ref, x_ref, xs_ref, flags_ref, out_ref, pair_ref, xt_ref, xst_ref):
    even = bit_of(0) == 0
    xt_ref[...] = x_ref[...].T
    xst_ref[...] = xs_ref[...].T

    @pl.when(even)
    def _():
        parts = tile(f_ref[...], g_ref[...], scale)
        flag = flag_of(flags_ref, 1)
        out_ref[...] = near_ref[...] + flag * times(parts, xs_ref[...])
        pair_ref[...] = times_back(parts, xt_ref[...]).astype(BF16)

    @pl.when(jnp.logical_not(even))
    def _():
        out_ref[...] = near_ref[...]
        pair_ref[...] = jnp.zeros_like(pair_ref)


def chunk_kernel(scale, size, f_ref, g_ref, far_ref, near_ref, xt_ref, xst_ref, flags_ref, *refs):
    even = lax.rem(lax.axis_index("leaf"), 2) == 0
    width = f_ref.shape[1]
    probes = near_ref.shape[1]
    heads = refs[: len(refs) // 5 * 3]
    out_ref, sib_ref, *back_refs = refs[len(heads) :]
    mine = flag_of(flags_ref, 2)

    def put(back, cross_back):
        if not heads:
            back_refs[0][...] = back
            back_refs[1][...] = jnp.zeros_like(back) if cross_back is None else cross_back
            return
        head = heads[1].shape[0]
        flag2 = far_ref[size : size + 1, :probes].astype(F32)
        flag1 = far_ref[size : size + 1, probes : 2 * probes].astype(F32)
        back_refs[0][:head] = (flag2 * heads[1][...] + flag1 * heads[2][...]).astype(BF16)
        total = flag2 * back
        back_refs[0][head:] = (total if cross_back is None else total + flag1 * cross_back).astype(BF16)

    @pl.when(even)
    def _():
        h = far_ref[:size, :width]
        xh = far_ref[:size, width:]
        parts = tile(f_ref[...], h, scale)
        out_ref[...] = near_ref[...] + mine * times(parts, xh)
        cross = tile(g_ref[...], h, scale)
        sib = times(cross, xh)
        sib_ref[...] = (sib + heads[0][...] if heads else sib).astype(sib_ref.dtype)
        put(times_back(parts, xt_ref[...]), times_back(cross, xst_ref[...]))

    @pl.when(jnp.logical_not(even))
    def _():
        h = far_ref[:size, :width]
        xh = far_ref[:size, width:]
        parts = tile(f_ref[...], h, scale)
        out_ref[...] = near_ref[...] + mine * times(parts, xh)
        sib_ref[...] = jnp.zeros_like(sib_ref)
        put(times_back(parts, xt_ref[...]), None)


def final_kernel(near_ref, far_ref, sib_ref, back_ref, flags_ref, out_ref):
    rows = out_ref.shape[0]
    after, before = flag_of(flags_ref, 1), flag_of(flags_ref, -1)
    sib = after * sib_ref[:rows].astype(F32) + before * sib_ref[rows : 2 * rows].astype(F32)
    out_ref[...] = near_ref[...] + far_ref[...] + sib + back_ref[...].astype(F32)


def sender(index, bits):
    return all(index >> at & 1 == bit for at, bit in bits)


def moved(array, by, wrap=True):
    peers = lax.axis_size("leaf")
    return lax.ppermute(array, "leaf", [(i, (i + by) % peers) for i in range(peers) if wrap or 0 <= i + by < peers])


def level1_partner(index):
    return index ^ (2 if index & 1 else 8 if index & 2 else 4)


def across(array, distance, bits=()):
    senders = [i for i in range(lax.axis_size("leaf")) if sender(i, bits)]
    return lax.ppermute(array, "leaf", [(i, i ^ distance) for i in senders])


def partner(array, level, bits=()):
    return across(array, 1 << level, bits)


def body(features, probes, bases, transfers, couplings, near_list, near_count):
    rows, width = features.shape
    lists = jnp.concatenate([near_list, near_count.reshape(1, 1)], axis=1)
    count = probes.shape[1]
    rank = bases.shape[1]
    depth = transfers.shape[1]
    scale = 1.0 / (rows * width)
    scale_g = (3.0 / rank) ** 0.5
    factors = [scale_g * 2.0 ** (-0.5 * (level + 1)) for level in range(depth)]
    shape = jax.ShapeDtypeStruct
    sizes = [rows * 6 // 8, rows * (8 - 6) // 8]

    sib_features = partner(features, 0)
    bases_v, transfer0 = call(
        load_kernel,
        [shape((rows, rank), F32), shape((rank, rank), F32)],
        [HBM] * 2,
        1000,
        bases, transfers,
        scratch=[pltpu.SemaphoreType.DMA((2,))],
        limit=LOAD_LIMIT,
    )
    (message,) = call(
        functools.partial(leaf_kernel, factors[0]),
        [shape((2 * count, rank), F32)],
        [VMEM] * 3,
        6 * rows * rank * count,
        bases_v, probes, transfer0,
    )
    gots = [partner(message, 0)]
    packed = []
    for at, more in enumerate(([], [lists])):
        packed += call(
            functools.partial(pack_kernel, sizes[0] * at),
            [shape((sizes[at] + FLAG_ROWS * at, width + count), BF16)]
            + [shape((FLAG_ROWS, count), F32), shape((rows, count), BF16)][: 2 * at],
            [VMEM] * (2 + len(more)),
            1000,
            features, probes, *more,
        )
    *packed, flags, own_x = packed
    sib_x = partner(own_x, 0)
    far_first = moved(packed[0], -2)
    far_last = moved(packed[1], -2, wrap=False)
    own = [message]
    for level in range(1, depth + 1):
        last = level == depth
        outs = [shape((count if last else 2 * count, rank), BF16), shape((count, rank), F32)]
        message, *own = call(
            functools.partial(up_kernel, level, None if last else factors[level]),
            outs[:1] if last else outs,
            [VMEM] * 3,
            6 * rank * rank * count,
            *own, gots[-1], transfers,
        )
        if level == 1:
            whole = [(i, level1_partner(i)) for i in range(lax.axis_size("leaf"))]
            gots.append(lax.ppermute(message, "leaf", whole))
        else:
            gots.append(partner(message, level, SHARED[min(level, 3)]))

    tile_flops = 2 * rows * rows * (width + 4 * count)
    (near,) = call(
        functools.partial(self_kernel, scale),
        [shape((rows, count), F32)],
        [VMEM, VMEM],
        tile_flops,
        features, probes,
    )
    near, pair, xt, xst = call(
        functools.partial(pair_kernel, scale),
        [shape((rows, count), F32), shape((rows, count), BF16)] + [shape((count, rows), BF16)] * 2,
        [VMEM] * 6,
        tile_flops,
        features, sib_features, near, own_x, sib_x, flags,
    )
    heads = []
    for at, (size, part) in enumerate(zip(sizes, (far_first, far_last))):
        back_shapes = [shape((size, count), F32)] * 2 if at == 0 else [shape((rows, count), BF16)]
        near, *heads = call(
            functools.partial(chunk_kernel, scale, size),
            [shape((rows, count), F32), shape((rows, count), BF16 if at else F32), *back_shapes],
            [VMEM] * (7 + len(heads)),
            tile_flops * 2 * size // rows,
            features, sib_features, part, near, xt, xst, flags, *heads,
        )
    cross, back = heads
    back = moved(back, 2, wrap=False)
    product_flops = 6 * count * rank * rank
    e3, e3_message = call(
        functools.partial(top_kernel, scale_g, factors[depth - 1]),
        [shape((count, rank), F32), shape((count, rank), BF16)],
        [VMEM] * 4,
        3 * product_flops,
        couplings, transfers, gots[depth - 1], gots[depth],
    )
    e3_sent = partner(e3_message, 2, SHARED[3])
    e2, e2_message = call(
        functools.partial(middle_kernel, scale_g, factors[2], 2),
        [shape((count, rank), F32), shape((count, rank), BF16)],
        [VMEM] * 5,
        2 * product_flops,
        couplings, transfers, gots[2], e3, e3_sent,
    )
    e2_sent = partner(e2_message, 1, SHARED[2])
    e1, sib_message = call(
        functools.partial(node_kernel, scale_g, factors[1], 1),
        [shape((count, rank), F32), shape((2 * rows + 2 * rank, count), BF16)],
        [VMEM] * 7,
        2 * product_flops,
        couplings, transfers, gots[1], e2, e2_sent, cross, pair,
    )
    sib_got = partner(sib_message, 0)
    (far_sum,) = call(
        functools.partial(down_kernel, scale_g, factors[0]),
        [shape((rows, count), F32)],
        [VMEM] * 6,
        2 * product_flops + 6 * rows * rank * count,
        couplings, transfers, bases_v, gots[0], e1, sib_got,
    )
    (out,) = call(
        final_kernel,
        [shape((rows, count), F32)],
        [VMEM] * 5,
        6 * rows * count,
        near, far_sum, sib_got, back, flags,
    )
    return out


def solution(mesh):
    in_specs = (
        P("leaf", None),
        P("leaf", None),
        P("leaf", None),
        P("leaf", None, None, None),
        P("leaf", None, None, None),
        P("leaf", None),
        P("leaf"),
    )
    out_specs = P("leaf", None)
    return jax.shard_map(body, mesh=mesh, in_specs=in_specs, out_specs=out_specs, check_vma=False)
```

```python
import functools

import jax
import jax.numpy as jnp
from jax import lax
from jax.experimental import pallas as pl
from jax.experimental.pallas import tpu as pltpu
from jax.sharding import PartitionSpec as P

BF16 = jnp.bfloat16
F32 = jnp.float32
VMEM = pl.BlockSpec(memory_space=pltpu.VMEM)
HBM = pl.BlockSpec(memory_space=pltpu.HBM)
ANY = pl.BlockSpec(memory_space=pl.ANY)
NN = (((1,), (0,)), ((), ()))
NT = (((1,), (1,)), ((), ()))
TN = (((0,), (0,)), ((), ()))
FLAG_ROWS = 8
OFFSETS = (-2, -1, 1, 2)
LIMIT = 16 << 20
LOAD_LIMIT = 55400000
SHARED = ((), ((0, 1),), ((0, 1), (1, 0)), ((0, 1), (1, 0), (2, 1)))


def dot(a, b, dims):
    return lax.dot_general(a, b, dims, preferred_element_type=F32)


def halves(a):
    high = a.astype(BF16)
    return high, (a - high.astype(F32)).astype(BF16)


def dot_wide(a, b, dims):
    a_high, a_low = halves(a)
    b_high, b_low = halves(b)
    return dot(a_high, b_high, dims) + (dot(a_high, b_low, dims) + dot(a_low, b_high, dims))


def dot_half(a16, b, dims):
    b_high, b_low = halves(b)
    return dot(a16, b_high, dims) + dot(a16, b_low, dims)


def member(near_list, near_count, offset):
    slots = lax.broadcasted_iota(jnp.int32, near_list.shape, 1)
    hits = (near_list == lax.axis_index("leaf") + offset) & (slots < near_count)
    return jnp.max(jnp.where(hits, jnp.float32(1.0), jnp.float32(0.0)), axis=1, keepdims=True)


def call(kernel, outs, specs, flops, *args, scratch=(), limit=LIMIT):
    out_bytes = sum(o.size * o.dtype.itemsize for o in outs)
    in_bytes = sum(a.size * a.dtype.itemsize for a in args)
    return pl.pallas_call(
        kernel,
        out_shape=outs,
        in_specs=specs,
        out_specs=[VMEM] * len(outs),
        scratch_shapes=list(scratch),
        compiler_params=pltpu.CompilerParams(vmem_limit_bytes=limit),
        cost_estimate=pl.CostEstimate(flops=flops, bytes_accessed=in_bytes + out_bytes, transcendentals=0),
    )(*args)


def load_kernel(bases_hbm, transfers_hbm, bases_ref, transfer_ref, sems):
    copies = [
        pltpu.make_async_copy(bases_hbm, bases_ref, sems.at[0]),
        pltpu.make_async_copy(transfers_hbm.at[0, 0], transfer_ref, sems.at[1]),
    ]
    for copy in copies:
        copy.start()
    for copy in copies:
        copy.wait()


def leaf_kernel(c1, bases_ref, x_ref, transfer_ref, message_ref):
    x = x_ref[...]
    probes = x.shape[1]
    skeleton = dot_wide(x, bases_ref[...], TN)
    message_ref[:probes] = skeleton
    message_ref[probes:] = c1 * dot_wide(skeleton, transfer_ref[...], NN)


def pack_kernel(first, f_ref, x_ref, *refs):
    rows, width = f_ref.shape
    probes = x_ref.shape[1]
    if len(refs) == 1:
        far_ref = refs[0]
        size = far_ref.shape[0]
    else:
        list_ref, far_ref, flags_ref, x16_ref = refs
        size = rows - first
        slots = list_ref.shape[1] - 1
        found = [member(list_ref[:, :slots], list_ref[:, slots:], offset) for offset in OFFSETS]
        flags = [jnp.broadcast_to(flag, (FLAG_ROWS, probes)) for flag in found[:2]]
        flags.append(jnp.zeros((FLAG_ROWS, width - probes), F32))
        far_ref[size:] = jnp.concatenate(flags, axis=1).astype(BF16)
        for row, flag in enumerate(found):
            flags_ref[row : row + 1] = jnp.broadcast_to(flag, (1, probes))
        x16_ref[...] = x_ref[...].astype(BF16)
    far_ref[:size, :width] = f_ref[first : first + size]
    far_ref[:size, width:] = x_ref[first : first + size].astype(BF16)


def flag_of(flags_ref, offset):
    row = OFFSETS.index(offset)
    return flags_ref[row : row + 1]


def up_kernel(level, factor, own_ref, got_ref, transfer_ref, message_ref, *next_refs):
    probes = message_ref.shape[0] if factor is None else message_ref.shape[0] // 2
    own = own_ref[probes : 2 * probes] if own_ref.shape[0] > probes else own_ref[...]
    skeleton = own + got_ref[probes : 2 * probes].astype(F32)
    message_ref[:probes] = skeleton.astype(message_ref.dtype)
    if factor is not None:
        moved = factor * dot_wide(skeleton, transfer_ref[0, level], NN)
        message_ref[probes:] = moved.astype(message_ref.dtype)
        next_refs[0][...] = moved


def bit_of(level):
    return lax.rem(lax.axis_index("leaf") >> level, 2)


def descend(scale_g, factor, got, coupling, transfer, above):
    wide = dot_wide if got.dtype == F32 else dot_half
    update = scale_g * wide(got, coupling, NT)
    return update if above is None else update + factor * dot_wide(above, transfer, NT)


def top_kernel(scale_g, factor, coupling_ref, transfer_ref, got_ref, root_ref, own_ref, message_ref):
    depth = transfer_ref.shape[1]
    probes = own_ref.shape[0]
    root = descend(scale_g, None, root_ref[...], coupling_ref[0, depth], None, None)
    out = descend(scale_g, factor, got_ref[:probes], coupling_ref[0, depth - 1], transfer_ref[0, depth - 1], root)
    own_ref[...] = out
    message_ref[...] = out.astype(BF16)


def middle_kernel(scale_g, factor, level, coupling_ref, transfer_ref, got_ref, above_ref, sent_ref, own_ref, message_ref):
    probes = own_ref.shape[0]
    above = jnp.where(bit_of(level) == 1, above_ref[...], sent_ref[...].astype(F32))
    out = descend(scale_g, factor, got_ref[:probes], coupling_ref[0, level], transfer_ref[0, level], above)
    own_ref[...] = out
    message_ref[...] = out.astype(BF16)


def node_kernel(scale_g, factor, level, coupling_ref, transfer_ref, got_ref, above_ref, sent_ref, cross_ref, pair_ref, own_ref, message_ref):
    probes, rank = own_ref.shape
    at = 2 * cross_ref.shape[0]
    message_ref[: at // 2] = cross_ref[...]
    message_ref[at // 2 : at] = pair_ref[...]
    above = jnp.where(bit_of(level) == 0, above_ref[...], sent_ref[...].astype(F32))
    out = descend(scale_g, factor, got_ref[:probes], coupling_ref[0, level], transfer_ref[0, level], above)
    own_ref[...] = out
    for part in halves(out):
        for first in range(0, rank, probes):
            message_ref[at : at + probes] = part[:, first : first + probes]
            at += probes


def down_kernel(scale_g, factor, coupling_ref, transfer_ref, bases_ref, got_ref, above_ref, sent_ref, near_ref, flags_ref, out_ref):
    rows, probes = out_ref.shape
    rank = bases_ref.shape[1]
    high, low = [
        jnp.concatenate([sent_ref[at + first : at + first + probes] for first in range(0, rank, probes)], axis=1).astype(F32)
        for at in (2 * rows, 2 * rows + rank)
    ]
    above = jnp.where(bit_of(0) == 1, above_ref[...], high + low)
    expansion = descend(scale_g, factor, got_ref[:probes], coupling_ref[0, 0], transfer_ref[0, 0], above)
    after, before = flag_of(flags_ref, 1), flag_of(flags_ref, -1)
    sib = after * sent_ref[:rows].astype(F32) + before * sent_ref[rows : 2 * rows].astype(F32)
    out_ref[...] = near_ref[...] + sib + dot_wide(bases_ref[...], expansion, NT)


def tile(rows_a, rows_b, scale):
    gram = dot(rows_a, rows_b, NT)
    return halves(gram * gram * scale)


def self_kernel(scale, f_ref, x_ref, out_ref):
    high, low = tile(f_ref[...], f_ref[...], scale)
    x_high, x_low = halves(x_ref[...])
    out_ref[...] = dot(high, x_high, NN) + (dot(high, x_low, NN) + dot(low, x_high, NN))


def times(parts, x16):
    return dot(parts[0], x16, NN) + dot(parts[1], x16, NN)


def times_back(parts, xt16):
    return (dot(xt16, parts[0], NN) + dot(xt16, parts[1], NN)).T


def pair_kernel(scale, f_ref, g_ref, near_ref, x_ref, xs_ref, flags_ref, out_ref, pair_ref, xt_ref, xst_ref):
    even = bit_of(0) == 0
    xt_ref[...] = x_ref[...].T
    xst_ref[...] = xs_ref[...].T

    @pl.when(even)
    def _():
        parts = tile(f_ref[...], g_ref[...], scale)
        flag = flag_of(flags_ref, 1)
        out_ref[...] = near_ref[...] + flag * times(parts, xs_ref[...])
        pair_ref[...] = times_back(parts, xt_ref[...]).astype(BF16)

    @pl.when(jnp.logical_not(even))
    def _():
        out_ref[...] = near_ref[...]
        pair_ref[...] = jnp.zeros_like(pair_ref)


def chunk_kernel(scale, size, f_ref, g_ref, far_ref, near_ref, xt_ref, xst_ref, flags_ref, *refs):
    even = lax.rem(lax.axis_index("leaf"), 2) == 0
    width = f_ref.shape[1]
    probes = near_ref.shape[1]
    heads = refs[: len(refs) // 5 * 3]
    out_ref, sib_ref, *back_refs = refs[len(heads) :]
    mine = flag_of(flags_ref, 2)

    def put(back, cross_back):
        if not heads:
            back_refs[0][...] = back
            back_refs[1][...] = jnp.zeros_like(back) if cross_back is None else cross_back
            return
        head = heads[1].shape[0]
        flag2 = far_ref[size : size + 1, :probes].astype(F32)
        flag1 = far_ref[size : size + 1, probes : 2 * probes].astype(F32)
        back_refs[0][:head] = (flag2 * heads[1][...] + flag1 * heads[2][...]).astype(BF16)
        total = flag2 * back
        back_refs[0][head:] = (total if cross_back is None else total + flag1 * cross_back).astype(BF16)

    @pl.when(even)
    def _():
        h = far_ref[:size, :width]
        xh = far_ref[:size, width:]
        parts = tile(f_ref[...], h, scale)
        out_ref[...] = near_ref[...] + mine * times(parts, xh)
        cross = tile(g_ref[...], h, scale)
        sib = times(cross, xh)
        sib_ref[...] = (sib + heads[0][...] if heads else sib).astype(sib_ref.dtype)
        put(times_back(parts, xt_ref[...]), times_back(cross, xst_ref[...]))

    @pl.when(jnp.logical_not(even))
    def _():
        h = far_ref[:size, :width]
        xh = far_ref[:size, width:]
        parts = tile(f_ref[...], h, scale)
        out_ref[...] = near_ref[...] + mine * times(parts, xh)
        sib_ref[...] = jnp.zeros_like(sib_ref)
        put(times_back(parts, xt_ref[...]), None)


def final_kernel(sum_ref, back_ref, out_ref):
    out_ref[...] = sum_ref[...] + back_ref[...].astype(F32)


def sender(index, bits):
    return all(index >> at & 1 == bit for at, bit in bits)


def moved(array, by, wrap=True):
    peers = lax.axis_size("leaf")
    return lax.ppermute(array, "leaf", [(i, (i + by) % peers) for i in range(peers) if wrap or 0 <= i + by < peers])


def level1_partner(index):
    return index ^ (2 if index & 1 else 4)


def across(array, distance, bits=()):
    senders = [i for i in range(lax.axis_size("leaf")) if sender(i, bits)]
    return lax.ppermute(array, "leaf", [(i, i ^ distance) for i in senders])


def partner(array, level, bits=()):
    return across(array, 1 << level, bits)


def body(features, probes, bases, transfers, couplings, near_list, near_count):
    rows, width = features.shape
    lists = jnp.concatenate([near_list, near_count.reshape(1, 1)], axis=1)
    count = probes.shape[1]
    rank = bases.shape[1]
    depth = transfers.shape[1]
    scale = 1.0 / (rows * width)
    scale_g = (3.0 / rank) ** 0.5
    factors = [scale_g * 2.0 ** (-0.5 * (level + 1)) for level in range(depth)]
    shape = jax.ShapeDtypeStruct
    sizes = [rows * 6 // 8, rows * (8 - 6) // 8]

    sib_features = partner(features, 0)
    bases_v, transfer0 = call(
        load_kernel,
        [shape((rows, rank), F32), shape((rank, rank), F32)],
        [HBM] * 2,
        1000,
        bases, transfers,
        scratch=[pltpu.SemaphoreType.DMA((2,))],
        limit=LOAD_LIMIT,
    )
    (message,) = call(
        functools.partial(leaf_kernel, factors[0]),
        [shape((2 * count, rank), F32)],
        [VMEM] * 3,
        6 * rows * rank * count,
        bases_v, probes, transfer0,
    )
    gots = [partner(message, 0)]
    packed = []
    for at, more in enumerate(([], [lists])):
        packed += call(
            functools.partial(pack_kernel, sizes[0] * at),
            [shape((sizes[at] + FLAG_ROWS * at, width + count), BF16)]
            + [shape((FLAG_ROWS, count), F32), shape((rows, count), BF16)][: 2 * at],
            [VMEM] * (2 + len(more)),
            1000,
            features, probes, *more,
        )
    *packed, flags, own_x = packed
    sib_x = partner(own_x, 0)
    far_first = moved(packed[0], -2)
    far_last = moved(packed[1], -2, wrap=False)
    own = [message]
    for level in range(1, depth + 1):
        last = level == depth
        outs = [shape((count if last else 2 * count, rank), BF16), shape((count, rank), F32)]
        message, *own = call(
            functools.partial(up_kernel, level, None if last else factors[level]),
            outs[:1] if last else outs,
            [VMEM] * 3,
            6 * rank * rank * count,
            *own, gots[-1], transfers,
        )
        if level == 1:
            whole = [(i, level1_partner(i)) for i in range(lax.axis_size("leaf"))]
            gots.append(lax.ppermute(message, "leaf", whole))
        else:
            gots.append(partner(message, level, SHARED[min(level, 3)]))

    tile_flops = 2 * rows * rows * (width + 4 * count)
    (near,) = call(
        functools.partial(self_kernel, scale),
        [shape((rows, count), F32)],
        [VMEM, VMEM],
        tile_flops,
        features, probes,
    )
    near, pair, xt, xst = call(
        functools.partial(pair_kernel, scale),
        [shape((rows, count), F32), shape((rows, count), BF16)] + [shape((count, rows), BF16)] * 2,
        [VMEM] * 6,
        tile_flops,
        features, sib_features, near, own_x, sib_x, flags,
    )
    heads = []
    for at, (size, part) in enumerate(zip(sizes, (far_first, far_last))):
        back_shapes = [shape((size, count), F32)] * 2 if at == 0 else [shape((rows, count), BF16)]
        near, *heads = call(
            functools.partial(chunk_kernel, scale, size),
            [shape((rows, count), F32), shape((rows, count), BF16 if at else F32), *back_shapes],
            [VMEM] * (7 + len(heads)),
            tile_flops * 2 * size // rows,
            features, sib_features, part, near, xt, xst, flags, *heads,
        )
    cross, back = heads
    back = moved(back, 2, wrap=False)
    product_flops = 6 * count * rank * rank
    e3, e3_message = call(
        functools.partial(top_kernel, scale_g, factors[depth - 1]),
        [shape((count, rank), F32), shape((count, rank), BF16)],
        [VMEM] * 4,
        3 * product_flops,
        couplings, transfers, gots[depth - 1], gots[depth],
    )
    e3_sent = partner(e3_message, 2, SHARED[3])
    e2, e2_message = call(
        functools.partial(middle_kernel, scale_g, factors[2], 2),
        [shape((count, rank), F32), shape((count, rank), BF16)],
        [VMEM] * 5,
        2 * product_flops,
        couplings, transfers, gots[2], e3, e3_sent,
    )
    e2_sent = partner(e2_message, 1, SHARED[2])
    e1, sib_message = call(
        functools.partial(node_kernel, scale_g, factors[1], 1),
        [shape((count, rank), F32), shape((2 * rows + 2 * rank, count), BF16)],
        [VMEM] * 7,
        2 * product_flops,
        couplings, transfers, gots[1], e2, e2_sent, cross, pair,
    )
    sib_got = partner(sib_message, 0)
    (far_sum,) = call(
        functools.partial(down_kernel, scale_g, factors[0]),
        [shape((rows, count), F32)],
        [VMEM] * 8,
        2 * product_flops + 6 * rows * rank * count,
        couplings, transfers, bases_v, gots[0], e1, sib_got, near, flags,
    )
    (out,) = call(
        final_kernel,
        [shape((rows, count), F32)],
        [VMEM] * 2,
        6 * rows * count,
        far_sum, back,
    )
    return out


def solution(mesh):
    in_specs = (
        P("leaf", None),
        P("leaf", None),
        P("leaf", None),
        P("leaf", None, None, None),
        P("leaf", None, None, None),
        P("leaf", None),
        P("leaf"),
    )
    out_specs = P("leaf", None)
    return jax.shard_map(body, mesh=mesh, in_specs=in_specs, out_specs=out_specs, check_vma=False)
```
